256 devices in a mesh: seq: 32 (over y_lo, z, core), head: 8 (over x, y_hi).
Axes of the slice: x: 4, y: 4 (y_hi: 2, y_lo: 2; y = y_hi * 2 + y_lo), z: 8, core: 2. Of those that a mesh axis runs over, the one named last changes fastest.
Arguments:
- prefix_embed: bfloat16 [256, 1024], replicated, may hold values from -6 to 6
- w_hidden: bfloat16 [1024, 8192], P(None, 'seq'), may hold values from -0.1875 to 0.1875
- b_hidden: float32 [8192], P('seq'), may hold values from -4 to 4
- w_out: bfloat16 [8192, 2, 1024], P('seq', None, 'head'), may hold values from -0.0625 to 0.0625
- queries: bfloat16 [4096, 8192], P('seq', 'head'), may hold values from -6 to 6
- keys: bfloat16 [4096, 1024], P('seq', 'head'), may hold values from -6 to 6
- values: bfloat16 [4096, 1024], P('seq', 'head'), may hold values from -6 to 6
- out_grad: bfloat16 [4096, 8192], P('seq', 'head'), may hold values from -6 to 6
Outputs:
- query_grad: bfloat16 [4096, 8192], P('seq', 'head')
- grad_w_out: float32 [8192, 2, 1024], P('seq', None, 'head')
- grad_w_hidden: float32 [1024, 8192], P(None, 'seq')
- grad_b_hidden: float32 [8192], P('seq')
- grad_prefix: float32 [256, 1024], replicated
The draws below stay inside these ranges and needn't reach their ends.
All inputs are finite; a program needn't handle non-finite values.
Results may differ from the reference program's by a relative error of at most 0.008.
Values may be sent and summed in bfloat16 or wider, within the bound.
No kernel may reach another device: no remote copies, remote signals or barrier semaphores. Data moves between devices by JAX's collectives and lax.ppermute only.
A program may use at most 64 MiB of HBM per device.

```python
import math
import jax
import jax.numpy as jnp
from jax import lax

QH = 64
KVH = 8
HD = 128
NPRE = 256
EMB = 1024
HID = 8192
LENGTH = 4096
TOKENS = 4096
SEQS = 1
Q_W = 8192
KV_W = 1024


def draw_queries(key, part):
    total_rows = TOKENS
    base = jnp.clip(jax.random.normal(jax.random.fold_in(key, 11), (total_rows, QH * HD), jnp.float32), -6.0, 6.0)
    return base.astype(jnp.bfloat16)


def draw_keys(key, part):
    total_rows = TOKENS
    base = jnp.clip(jax.random.normal(jax.random.fold_in(key, 23), (total_rows, KVH * HD), jnp.float32), -6.0, 6.0)
    return base.astype(jnp.bfloat16)


def shard_levels(rng, dims, cuts, smallest, high):
    level = 1.0
    for position, shards_of in cuts:
        steps = jax.random.uniform(jax.random.fold_in(jax.random.fold_in(rng, 6), position), (shards_of,), jnp.float32, smallest / len(cuts), high / len(cuts))
        level = level * jnp.repeat(jnp.exp(steps), dims[position] // shards_of).reshape((-1,) + (1,) * (len(dims) - 1 - position))
    return level


def noise(stream_key, shape, width, most, cuts=(), held_as=jnp.bfloat16):
    loudness = shard_levels(stream_key, shape, cuts, -0.22, 0.18) if cuts else 1.0
    drawn = jax.random.normal(stream_key, shape, jnp.float32) * width * loudness
    return jnp.minimum(jnp.maximum(drawn, -most), most).astype(held_as)


def setup_inputs(seed: int = 0) -> dict:
    splits = jax.random.split(jax.random.key(seed), 9)
    prefix_embed = noise(splits[0], (NPRE, EMB), 1.0, 6.0)
    w_hidden = noise(splits[1], (EMB, HID), EMB ** -0.5, 0.1875, ((1, 32),))
    b_hidden = noise(splits[2], (HID,), 1.0, 4.0, ((0, 32),), jnp.float32)
    w_out = noise(splits[3], (HID, 2, KV_W), HID ** -0.5, 0.0625, ((0, 32), (2, 8)))
    queries = draw_queries(jax.random.fold_in(splits[8], 71), 0)
    keys = draw_keys(jax.random.fold_in(splits[8], 71), 0)
    values = noise(splits[6], (TOKENS, KV_W), 1.0, 6.0, ((0, 32), (1, 8)))
    out_grad = noise(splits[7], (TOKENS, Q_W), 1.0, 6.0, ((0, 32), (1, 8)))
    return dict(prefix_embed=prefix_embed, w_hidden=w_hidden, b_hidden=b_hidden, w_out=w_out, queries=queries, keys=keys, values=values, out_grad=out_grad)


def reference(prefix_embed, w_hidden, b_hidden, w_out, queries, keys, values, out_grad):
    scaling = 1.0 / math.sqrt(HD)
    group = QH // KVH
    hidden_pre = jnp.dot(prefix_embed, w_hidden, preferred_element_type=jnp.float32) + b_hidden
    tangent = jnp.tanh(hidden_pre)
    hidden = tangent.astype(jnp.bfloat16)
    prefix_kv = jnp.einsum('ph,hck->pck', hidden.astype(jnp.float32), w_out.astype(jnp.float32)).astype(jnp.bfloat16)
    prefix_keys = prefix_kv[:, 0]
    prefix_values = prefix_kv[:, 1]
    positions = jnp.arange(LENGTH, dtype=jnp.int32)
    causal = positions[None, :] <= positions[:, None]
    visible = jnp.concatenate([jnp.ones((LENGTH, NPRE), dtype=bool), causal], 1)

    def one_sequence(pieces):
        seq_queries, seq_keys, seq_values, seq_grads = pieces

        def one_head(head):
            kv_head = head // group
            query_rows = lax.dynamic_slice_in_dim(seq_queries, (head * HD).astype(jnp.int32), HD, 1)
            grad_rows = lax.dynamic_slice_in_dim(seq_grads, (head * HD).astype(jnp.int32), HD, 1)
            column = (kv_head * HD).astype(jnp.int32)
            key_all = jnp.concatenate([lax.dynamic_slice_in_dim(prefix_keys, column, HD, 1), lax.dynamic_slice_in_dim(seq_keys, column, HD, 1)], 0)
            value_all = jnp.concatenate([lax.dynamic_slice_in_dim(prefix_values, column, HD, 1), lax.dynamic_slice_in_dim(seq_values, column, HD, 1)], 0)
            logits = jnp.dot(query_rows, key_all.T, preferred_element_type=jnp.float32) * scaling
            logits = jnp.where(visible, logits, -jnp.inf)
            row_max = lax.optimization_barrier(jnp.max(logits, axis=1, keepdims=True))
            log_total = row_max + jnp.log(lax.optimization_barrier(jnp.sum(jnp.exp(logits - row_max), axis=1, keepdims=True)))
            probs = jnp.exp(logits - log_total)
            dot_grads = jnp.dot(grad_rows, value_all.T, preferred_element_type=jnp.float32)
            delta_row = lax.optimization_barrier(jnp.sum(probs * dot_grads, axis=1, keepdims=True))
            score_grad = (probs * (dot_grads - delta_row)).astype(jnp.bfloat16)
            probs_b = probs.astype(jnp.bfloat16)
            head_grad = (jnp.dot(score_grad, key_all, preferred_element_type=jnp.float32) * scaling).astype(jnp.bfloat16)
            key_grad = jnp.dot(score_grad[:, :NPRE].T, query_rows, preferred_element_type=jnp.float32) * scaling
            value_grad = jnp.dot(probs_b[:, :NPRE].T, grad_rows, preferred_element_type=jnp.float32)
            return (head_grad, key_grad, value_grad)
        head_grads, key_grads, value_grads = lax.map(one_head, jnp.arange(QH, dtype=jnp.int32))
        seq_query_grad = head_grads.transpose(1, 0, 2).reshape(LENGTH, QH * HD)
        key_sum = key_grads.reshape(KVH, group, NPRE, HD).sum(1).transpose(1, 0, 2).reshape(NPRE, KVH * HD)
        value_sum = value_grads.reshape(KVH, group, NPRE, HD).sum(1).transpose(1, 0, 2).reshape(NPRE, KVH * HD)
        return (seq_query_grad, key_sum, value_sum)
    stacked = (queries.reshape(SEQS, LENGTH, QH * HD), keys.reshape(SEQS, LENGTH, KVH * HD), values.reshape(SEQS, LENGTH, KVH * HD), out_grad.reshape(SEQS, LENGTH, QH * HD))
    seq_grads, key_sums, value_sums = lax.map(one_sequence, stacked)
    query_grad = seq_grads.reshape(SEQS * LENGTH, QH * HD)
    prefix_grads = jnp.stack([lax.optimization_barrier(jnp.sum(key_sums, axis=0)), lax.optimization_barrier(jnp.sum(value_sums, axis=0))], 1).astype(jnp.bfloat16)
    grad_w_out = jnp.einsum('ph,pck->hck', hidden.astype(jnp.float32), prefix_grads.astype(jnp.float32))
    hidden_grad = jnp.einsum('pck,hck->ph', prefix_grads.astype(jnp.float32), w_out.astype(jnp.float32))
    pre_grad = hidden_grad * (1.0 - tangent * tangent)
    pre_rounded = pre_grad.astype(jnp.bfloat16)
    grad_w_hidden = jnp.dot(prefix_embed.T, pre_rounded, preferred_element_type=jnp.float32)
    grad_b_hidden = lax.optimization_barrier(jnp.sum(pre_grad, axis=0))
    grad_prefix = jnp.dot(pre_rounded, w_hidden.T, preferred_element_type=jnp.float32)
    return (query_grad, grad_w_out, grad_w_hidden, grad_b_hidden, grad_prefix)
```

```python
import math

import jax
import jax.numpy as jnp
from jax import lax
from jax.experimental import pallas as pl
from jax.experimental.pallas import tpu as pltpu
from jax.sharding import Mesh
from jax.sharding import PartitionSpec as P

HD = 128
SCALE = 1.0 / math.sqrt(HD)
LOG2E = math.log2(math.e)
C1 = SCALE * LOG2E
NEG = -1e30
SEQ = ("y", "z", "c")
YZ = ("y", "z")
CYZ = ("c", "y", "z")
HEAD = ("x", "w")
OWNERS = ("x", "w", "y", "z")
F32 = jnp.float32
BF16 = jnp.bfloat16


def dot_nt(a, b):
    return lax.dot_general(a, b, (((1,), (1,)), ((), ())), preferred_element_type=F32)


def dot_nn(a, b):
    return lax.dot_general(a, b, (((1,), (0,)), ((), ())), preferred_element_type=F32)


def dot_tn(a, b):
    return lax.dot_general(a, b, (((0,), (0,)), ((), ())), preferred_element_type=F32)


def stats_kernel(pos, q, g, own_k, own_v, mine, other, pkv, grads, stats, q2, g2):
    rows = own_k.shape[0]
    heads = q.shape[1] // HD
    tile = 2 * HD
    tiles = heads * rows // tile
    npre = pkv.shape[1]
    here = pos[0]
    core = pos[1]
    for h in range(heads):
        q2[h * rows : (h + 1) * rows, :] = q[:, h * HD : (h + 1) * HD]
        g2[h * rows : (h + 1) * rows, :] = g[:, h * HD : (h + 1) * HD]

    def update(state, s, d):
        m, l, t = state
        n = s.shape[0] // 8
        s = s.reshape(n, 8, tile)
        d = d.reshape(n, 8, tile)
        new = jnp.maximum(m, jnp.max(s, axis=0))
        fade = jnp.exp2(m - new)
        w = jnp.exp2(s - new[None])
        return (new, l * fade + jnp.sum(w, axis=0), t * fade + jnp.sum(w * d, axis=0))

    def tile_of(r):
        return slice(r * tile, (r + 1) * tile)

    def sweep(i, states):
        kc = jnp.concatenate([mine[i, 0], other[i, 0]], 0)
        vc = jnp.concatenate([mine[i, 1], other[i, 1]], 0)
        out = []
        for r in range(tiles):
            s = dot_nt(kc, q2[tile_of(r), :]) * C1
            d = dot_nt(vc, g2[tile_of(r), :])
            out.append(update(states[r], s, d))
        return tuple(out)

    zero = jnp.zeros((8, tile), F32)
    states = tuple((jnp.full((8, tile), NEG, F32), zero, zero) for _ in range(tiles))
    states = lax.fori_loop(0, here, sweep, states)
    kc = jnp.concatenate([own_k[...], other[here, 0]], 0)
    vc = jnp.concatenate([own_v[...], other[here, 1]], 0)
    key = lax.broadcasted_iota(jnp.int32, (2 * rows, tile), 0)
    row = lax.broadcasted_iota(jnp.int32, (2 * rows, tile), 1) % rows
    bound = jnp.where(key < rows, row, rows - 1 + core * rows)
    seen = key <= bound
    kg = jnp.zeros((npre, HD), F32)
    vg = jnp.zeros((npre, HD), F32)
    for r in range(tiles):
        s = jnp.where(seen, dot_nt(kc, q2[tile_of(r), :]) * C1, NEG)
        d = dot_nt(vc, g2[tile_of(r), :])
        state = update(states[r], s, d)
        s = dot_nt(pkv[0], q2[tile_of(r), :]) * C1
        d = dot_nt(pkv[1], g2[tile_of(r), :])
        m, l, t = update(state, s, d)
        top = jnp.max(m, axis=0, keepdims=True)
        fade = jnp.exp2(m - top)
        total = jnp.sum(l * fade, axis=0, keepdims=True)
        delta = jnp.sum(t * fade, axis=0, keepdims=True) / total
        log_total = top + jnp.log2(total)
        stats[0:1, tile_of(r)] = log_total
        stats[1:2, tile_of(r)] = delta
        p = jnp.exp2(s - log_total)
        ds = (p * (d - delta)).astype(BF16)
        kg = kg + dot_nn(ds, q2[tile_of(r), :])
        vg = vg + dot_nn(p.astype(BF16), g2[tile_of(r), :])
    grads[0] = (kg * SCALE).astype(grads.dtype)
    grads[1] = vg.astype(grads.dtype)


def grad_kernel(pos, q, g, stats, own_k, own_v, mine, other, pkv, *rest):
    out, q2, g2, lt, de = rest[-5:]
    rows = own_k.shape[0]
    heads = q.shape[1] // HD
    tile = heads * rows
    here = pos[0]
    core = pos[1]
    for h in range(heads):
        span = slice(h * rows, (h + 1) * rows)
        q2[span, :] = q[:, h * HD : (h + 1) * HD]
        g2[span, :] = g[:, h * HD : (h + 1) * HD]
    lt[...] = jnp.broadcast_to(stats[:, 0:1], (tile, HD))
    de[...] = jnp.broadcast_to(stats[:, 1:2], (tile, HD))

    def part(kc, vc, seen=None):
        s = dot_nt(q2[...], kc) * C1
        d = dot_nt(g2[...], vc)
        if seen is not None:
            s = jnp.where(seen, s, NEG)
        pieces = []
        for b in range(kc.shape[0] // HD):
            lanes = slice(b * HD, (b + 1) * HD)
            p = jnp.exp2(s[:, lanes] - lt[...])
            pieces.append((p * (d[:, lanes] - de[...])).astype(BF16))
        return dot_nn(jnp.concatenate(pieces, 1), kc)

    def sweep(i, total):
        kc = jnp.concatenate([mine[i, 0], other[i, 0]], 0)
        vc = jnp.concatenate([mine[i, 1], other[i, 1]], 0)
        return total + part(kc, vc)

    total = part(pkv[0], pkv[1])
    total = lax.fori_loop(0, here, sweep, total)
    kc = jnp.concatenate([own_k[...], other[here, 0]], 0)
    vc = jnp.concatenate([own_v[...], other[here, 1]], 0)
    key = lax.broadcasted_iota(jnp.int32, (tile, 2 * rows), 1)
    row = lax.broadcasted_iota(jnp.int32, (tile, 2 * rows), 0) % rows
    bound = jnp.where(key < rows, row, rows - 1 + core * rows)
    total = (total + part(kc, vc, key <= bound)) * SCALE
    for h in range(heads):
        out[:, h * HD : (h + 1) * HD] = total[h * rows : (h + 1) * rows].astype(out.dtype)


def whole(shape):
    return pl.BlockSpec(shape, lambda *_: (0,) * len(shape))


def attention_stats(pos, q, g, own_k, own_v, mine, other, pkv):
    rows, width = q.shape
    n = rows * width // HD
    return pl.pallas_call(
        stats_kernel,
        out_shape=(
            jax.ShapeDtypeStruct(pkv.shape, BF16),
            jax.ShapeDtypeStruct((2, n), F32),
        ),
        in_specs=[pl.BlockSpec(memory_space=pltpu.SMEM)]
        + [whole(v.shape) for v in (q, g, own_k, own_v, mine, other, pkv)],
        out_specs=(whole(pkv.shape), whole((2, n))),
        grid=(1,),
        scratch_shapes=[
            pltpu.VMEM((n, HD), BF16),
            pltpu.VMEM((n, HD), BF16),
        ],
        cost_estimate=pl.CostEstimate(flops=3 * 10**9, bytes_accessed=3 * 10**6, transcendentals=4 * 10**6),
        name="stats",
    )(pos, q, g, own_k, own_v, mine, other, pkv)


def query_grad_piece(piece, count, pos, q, g, stats, own_k, own_v, mine, other, pkv, *prior):
    rows, width = q.shape
    part = width // count
    tile = part // HD * rows
    block = pl.BlockSpec((rows, part), lambda *_: (0, piece))
    return pl.pallas_call(
        grad_kernel,
        out_shape=jax.ShapeDtypeStruct(q.shape, BF16),
        in_specs=[
            pl.BlockSpec(memory_space=pltpu.SMEM),
            block,
            block,
            pl.BlockSpec((tile, 2), lambda *_: (piece, 0)),
        ]
        + [whole(v.shape) for v in (own_k, own_v, mine, other, pkv)]
        + [pl.BlockSpec(memory_space=pl.ANY) for _ in prior],
        out_specs=block,
        grid=(1,),
        scratch_shapes=[
            pltpu.VMEM((tile, HD), BF16),
            pltpu.VMEM((tile, HD), BF16),
            pltpu.VMEM((tile, HD), F32),
            pltpu.VMEM((tile, HD), F32),
        ],
        input_output_aliases={9: 0} if prior else {},
        cost_estimate=pl.CostEstimate(flops=10**9, bytes_accessed=3 * 10**6, transcendentals=10**6),
        name="query_grad",
    )(pos, q, g, stats, own_k, own_v, mine, other, pkv, *prior)


def exchange(value, axes):
    return lax.all_to_all(value, axes, 0, 0, tiled=True)


def to_all(value, axes):
    return exchange(jnp.broadcast_to(value, (lax.axis_size(axes), *value.shape)), axes)


def sum_parts(value, axes, dtype=BF16):
    count = lax.axis_size(axes)
    parts = exchange(value.reshape(count, -1, HD).astype(dtype), axes)
    return jnp.sum(parts.astype(F32), axis=0)


def sum_everywhere(value):
    own = sum_parts(value, SEQ).astype(BF16)
    return to_all(own, SEQ).reshape(value.shape)


def swap_cores(value):
    return lax.ppermute(value, "c", [(0, 1), (1, 0)])


def on_device(prefix_embed, w_hidden, b_hidden, w_out, queries, keys, values, out_grad):
    npre, emb = prefix_embed.shape
    units = w_hidden.shape[1]
    core = lax.axis_index("c")
    here = lax.axis_index(YZ)
    head = lax.axis_index(HEAD)
    heads = lax.axis_size(HEAD)
    pos = jnp.stack([here, core]).astype(jnp.int32)

    mine = to_all(jnp.stack([keys, values], 0), YZ)
    hidden_pre = jnp.dot(prefix_embed, w_hidden, preferred_element_type=F32) + b_hidden
    tangent = jnp.tanh(hidden_pre)
    hidden = tangent.astype(BF16)
    partial_kv = jnp.einsum("ph,hck->cpk", hidden, w_out, preferred_element_type=F32)
    pkv = sum_everywhere(partial_kv)
    other = swap_cores(mine)
    grads, stats = attention_stats(pos, queries, out_grad, keys, values, mine, other, pkv)
    columns = stats.T
    prefix_grads = sum_everywhere(grads)
    query_grad = ()
    count = 4
    for piece in range(count):
        query_grad = (
            query_grad_piece(
                piece, count, pos, queries, out_grad, columns, keys, values, mine, other, pkv, *query_grad
            ),
        )
    grad_w_out = jnp.einsum("ph,cpk->hck", hidden, prefix_grads, preferred_element_type=F32)
    hidden_part = jnp.einsum("cpk,hck->ph", prefix_grads, w_out, preferred_element_type=F32)
    share = npre // heads
    parts = exchange(hidden_part.reshape(heads, share, units), HEAD)
    hidden_grad = jnp.sum(parts, axis=0)
    own_tangent = lax.dynamic_slice_in_dim(tangent, head * share, share, 0)
    pre_part = (hidden_grad * (1.0 - own_tangent * own_tangent)).astype(BF16)
    embed_part = dot_nt(pre_part, w_hidden)
    own = sum_parts(embed_part, CYZ)
    near = to_all(own.astype(BF16), OWNERS)
    far = swap_cores(near)
    sides = jnp.stack([jnp.where(core == 0, near, far), jnp.where(core == 0, far, near)], 0)
    sides = sides.reshape(2, heads, -1, emb).transpose(1, 0, 2, 3)
    grad_prefix = sides.reshape(npre, emb).astype(F32)
    pre_rounded = to_all(pre_part, HEAD).reshape(npre, units)
    grad_w_hidden = dot_tn(prefix_embed, pre_rounded)
    grad_b_hidden = jnp.sum(pre_rounded.astype(F32), axis=0)
    return (*query_grad, grad_w_out, grad_w_hidden, grad_b_hidden, grad_prefix)


def solution(mesh):
    torus = Mesh(mesh.devices.reshape(2, 8, 2, 4, 2), ("y", "z", "c", "x", "w"))
    placed = (
        P(),
        P(None, SEQ),
        P(SEQ),
        P(SEQ, None, HEAD),
        P(SEQ, HEAD),
        P(SEQ, HEAD),
        P(SEQ, HEAD),
        P(SEQ, HEAD),
    )
    return jax.shard_map(
        on_device,
        mesh=torus,
        in_specs=placed,
        out_specs=(P(SEQ, HEAD), P(SEQ, None, HEAD), P(None, SEQ), P(SEQ), P()),
        check_vma=False,
    )
```

```python
import functools
import math

import jax
import jax.numpy as jnp
from jax import lax
from jax.experimental import pallas as pl
from jax.experimental.pallas import tpu as pltpu
from jax.sharding import Mesh
from jax.sharding import PartitionSpec as P

HD = 128
SCALE = 1.0 / math.sqrt(HD)
C1 = SCALE * math.log2(math.e)
NEG = -1e30
TILE = 256
PIECES = 4
SEQ = ("y", "z", "c")
YZ = ("y", "z")
CYZ = ("c", "y", "z")
HEAD = ("x", "w")
OWNERS = ("x", "w", "y", "z")
F32 = jnp.float32
BF16 = jnp.bfloat16
SMEM = pl.BlockSpec(memory_space=pltpu.SMEM)
VMEM = pl.BlockSpec(memory_space=pltpu.VMEM)


def dot_nt(a, b):
    return lax.dot_general(a, b, (((1,), (1,)), ((), ())), preferred_element_type=F32)


def dot_nn(a, b):
    return lax.dot_general(a, b, (((1,), (0,)), ((), ())), preferred_element_type=F32)


def dot_tn(a, b):
    return lax.dot_general(a, b, (((0,), (0,)), ((), ())), preferred_element_type=F32)


def span(r):
    return slice(r * TILE, (r + 1) * TILE)


def update(state, s, d):
    m, l, t = state
    s = s.reshape(-1, 8, TILE)
    d = d.reshape(-1, 8, TILE)
    new = jnp.maximum(m, jnp.max(s, axis=0))
    fade = jnp.exp2(m - new)
    w = jnp.exp2(s - new[None])
    return (new, l * fade + jnp.sum(w, axis=0), t * fade + jnp.sum(w * d, axis=0))


def pair_of(kv, j):
    k = jnp.concatenate([kv[2 * j, :HD], kv[2 * j + 1, :HD]], 0)
    v = jnp.concatenate([kv[2 * j, HD : 2 * HD], kv[2 * j + 1, HD : 2 * HD]], 0)
    return k, v


def visible(pos, own, j, shape, key_dim):
    key = lax.broadcasted_iota(jnp.int32, shape, key_dim)
    row = lax.broadcasted_iota(jnp.int32, shape, 1 - key_dim) % HD
    if own:
        return key <= (pos[0] - 2 * j) * HD + row
    return key < (pos[0] + pos[1] - 2 * j) * HD


def sweep_kernel(pos, q, g, mine, other, out):
    tiles = q.shape[0] // TILE

    def step(j, states, masked=False):
        for own, kv in ((True, mine), (False, other)):
            k, v = pair_of(kv, j)
            seen = visible(pos, own, j, (2 * HD, TILE), 0) if masked else None
            new = []
            for r in range(tiles):
                s = dot_nt(k, q[span(r), :]) * C1
                if masked:
                    s = jnp.where(seen, s, NEG)
                new.append(update(states[r], s, dot_nt(v, g[span(r), :])))
            states = tuple(new)
        return states

    zero = jnp.zeros((8, TILE), F32)
    states = tuple((jnp.full((8, TILE), NEG, F32), zero, zero) for _ in range(tiles))
    half = pos[0] // 2
    states = step(half, lax.fori_loop(0, half, step, states), True)
    for r in range(tiles):
        for a in range(3):
            out[a, :, span(r)] = states[r][a]


def prefix_kernel(q, g, pkv, state, grads, stats):
    npre = pkv.shape[1]
    kg = jnp.zeros((npre, HD), F32)
    vg = jnp.zeros((npre, HD), F32)
    for r in range(q.shape[0] // TILE):
        s = dot_nt(pkv[0], q[span(r), :]) * C1
        d = dot_nt(pkv[1], g[span(r), :])
        m, l, t = update(tuple(state[a, :, span(r)] for a in range(3)), s, d)
        top = jnp.max(m, axis=0, keepdims=True)
        fade = jnp.exp2(m - top)
        total = jnp.sum(l * fade, axis=0, keepdims=True)
        delta = jnp.sum(t * fade, axis=0, keepdims=True) / total
        log_total = top + jnp.log2(total)
        stats[0:1, span(r)] = log_total
        stats[1:2, span(r)] = delta
        p = jnp.exp2(s - log_total)
        kg = kg + dot_nn((p * (d - delta)).astype(BF16), q[span(r), :])
        vg = vg + dot_nn(p.astype(BF16), g[span(r), :])
    grads[0] = (kg * SCALE).astype(grads.dtype)
    grads[1] = vg.astype(grads.dtype)


def grad_kernel(piece, pos, q, g, stats, mine, other, extra, out, total, log_total, delta):
    rows = q.shape[0]
    columns = stats[...].T
    log_total[...] = jnp.broadcast_to(columns[:, 0:1], (rows, HD))
    delta[...] = jnp.broadcast_to(columns[:, 1:2], (rows, HD))

    def part(k, v, seen=None):
        for r in range(rows // TILE):
            s = dot_nt(q[span(r), :], k) * C1
            if seen is not None:
                s = jnp.where(seen, s, NEG)
            d = dot_nt(g[span(r), :], v)
            pieces = []
            for b in range(k.shape[0] // HD):
                lanes = slice(b * HD, (b + 1) * HD)
                p = jnp.exp2(s[:, lanes] - log_total[span(r), :])
                pieces.append((p * (d[:, lanes] - delta[span(r), :])).astype(BF16))
            total[span(r), :] += dot_nn(jnp.concatenate(pieces, 1), k)

    def step(i, masked=False):
        for own, kv in ((True, mine), (False, other)):
            k, v = pair_of(kv, i)
            seen = visible(pos, own, first + i, (TILE, 2 * HD), 1) if masked else None
            part(k, v, seen)

    if piece == 0:
        total[...] = jnp.zeros((rows, HD), F32)
        part(extra[0], extra[1])
    else:
        total[...] = extra[...]
    pairs = mine.shape[0] // 2
    first = piece * pairs
    half = pos[0] // 2
    lax.fori_loop(0, jnp.clip(half - first, 0, pairs), lambda i, _: step(i), None)

    @pl.when((half >= first) & (half < first + pairs))
    def _():
        step(half - first, True)

    if piece < PIECES - 1:
        out[...] = total[...]
    else:
        result = (total[...] * SCALE).astype(out.dtype)
        for h in range(rows // HD):
            out[:, h * HD : (h + 1) * HD] = result[h * HD : (h + 1) * HD]


def sweep(pos, q, g, mine, other):
    return pl.pallas_call(
        sweep_kernel,
        out_shape=jax.ShapeDtypeStruct((3, 8, q.shape[0]), F32),
        in_specs=[SMEM] + [VMEM] * 4,
        out_specs=VMEM,
        cost_estimate=pl.CostEstimate(flops=2 * 10**9, bytes_accessed=3 * 10**6, transcendentals=4 * 10**6),
        name="sweep",
    )(pos, q, g, mine, other)


def prefix_part(q, g, pkv, state):
    return pl.pallas_call(
        prefix_kernel,
        out_shape=(
            jax.ShapeDtypeStruct(pkv.shape, BF16),
            jax.ShapeDtypeStruct((2, q.shape[0]), F32),
        ),
        in_specs=[VMEM] * 4,
        out_specs=(VMEM, VMEM),
        cost_estimate=pl.CostEstimate(flops=3 * 10**8, bytes_accessed=10**6, transcendentals=5 * 10**5),
        name="prefix_part",
    )(q, g, pkv, state)


def whole(value):
    return pl.BlockSpec(value.shape, lambda *_: (0,) * value.ndim)


def query_grad_piece(piece, pos, q, g, stats, mine, other, extra):
    n = q.shape[0]
    blocks, *shape = mine.shape
    part = pl.BlockSpec((blocks // PIECES, *shape), lambda *_: (piece, 0, 0))
    out = jax.ShapeDtypeStruct((n, HD), F32)
    if piece == PIECES - 1:
        out = jax.ShapeDtypeStruct((HD, n), BF16)
    return pl.pallas_call(
        functools.partial(grad_kernel, piece),
        out_shape=out,
        in_specs=[SMEM, whole(q), whole(g), whole(stats), part, part, whole(extra)],
        out_specs=whole(out),
        grid=(1,),
        scratch_shapes=[pltpu.VMEM((n, HD), F32)] * 3,
        cost_estimate=pl.CostEstimate(flops=10**9, bytes_accessed=3 * 10**6, transcendentals=10**6),
        name="query_grad",
    )(pos, q, g, stats, mine, other, extra)


def exchange(value, axes):
    return lax.all_to_all(value, axes, 0, 0, tiled=True)


def to_all(value, axes):
    return exchange(jnp.broadcast_to(value, (lax.axis_size(axes), *value.shape)), axes)


def sum_parts(value, axes, dtype=BF16):
    parts = exchange(value.reshape(lax.axis_size(axes), -1, HD).astype(dtype), axes)
    return jnp.sum(parts.astype(F32), axis=0)


def shift(value, axis, steps):
    count = lax.axis_size(axis)
    return lax.ppermute(value, axis, [(i, (i + steps) % count) for i in range(count)])


def by_head(rows):
    return rows.reshape(rows.shape[0], -1, HD).transpose(1, 0, 2).reshape(-1, HD)


def on_device(prefix_embed, w_hidden, b_hidden, w_out, queries, keys, values, out_grad):
    npre, emb = prefix_embed.shape
    units = w_hidden.shape[1]
    core = lax.axis_index("c")
    here = lax.axis_index(YZ)
    head = lax.axis_index(HEAD)
    heads = lax.axis_size(HEAD)
    share = npre // heads
    pos = jnp.stack([here, core]).astype(jnp.int32)

    hidden_pre = jnp.dot(prefix_embed, w_hidden, preferred_element_type=F32) + b_hidden
    tangent = jnp.tanh(hidden_pre)
    hidden = tangent.astype(BF16)
    partial_kv = jnp.einsum("ph,hck->cpk", hidden, w_out, preferred_element_type=F32)
    groups = lax.axis_size(YZ)
    kv = jnp.concatenate([keys, values], 0)
    partial_kv = partial_kv.reshape(groups, -1, HD).astype(BF16)
    mine = exchange(jnp.concatenate([jnp.broadcast_to(kv, (groups, *kv.shape)), partial_kv], 1), YZ)
    own = jnp.sum(mine[:, kv.shape[0] :].astype(F32), axis=0)
    own = (own + shift(own, "c", 1)).astype(BF16)
    other = shift(mine, "c", 1)
    pkv = to_all(own, YZ).reshape(2, npre, HD)
    q = by_head(queries)
    g = by_head(out_grad)
    state = sweep(pos, q, g, mine, other)
    grads, stats = prefix_part(q, g, pkv, state)
    own_grads = sum_parts(grads, SEQ).astype(BF16)
    prefix_grads = to_all(own_grads, SEQ).reshape(2, npre, HD)
    query_grad = pkv
    for piece in range(PIECES):
        query_grad = query_grad_piece(piece, pos, q, g, stats, mine, other, query_grad)
    grad_w_out = jnp.einsum("ph,cpk->hck", hidden, prefix_grads, preferred_element_type=F32)
    hidden_part = jnp.einsum("cpk,hck->ph", prefix_grads, w_out, preferred_element_type=F32)
    parts = exchange(hidden_part.reshape(heads, share, units), HEAD)
    hidden_grad = jnp.sum(parts, axis=0)
    own_tangent = lax.dynamic_slice_in_dim(tangent, head * share, share, 0)
    pre_part = (hidden_grad * (1.0 - own_tangent * own_tangent)).astype(BF16)
    embed_part = dot_nt(pre_part, w_hidden)
    own_embed = sum_parts(embed_part, CYZ).astype(BF16)
    near = to_all(own_embed, OWNERS)
    far = shift(near, "c", 1)
    sides = jnp.stack([jnp.where(core == 0, near, far), jnp.where(core == 0, far, near)], 0)
    sides = sides.reshape(2, heads, -1, emb).transpose(1, 0, 2, 3)
    grad_prefix = sides.reshape(npre, emb).astype(F32)
    both = jnp.concatenate([pre_part, shift(pre_part, "w", 1)], 0)
    lines = lax.axis_size("x")
    pre_rounded = jnp.concatenate([both] + [shift(both, "x", k) for k in range(1, lines)], 0)
    x, w = lax.axis_index("x"), lax.axis_index("w")
    order = []
    for k in range(lines):
        for other_w in (w, 1 - w):
            source = (x - k) % lines * lax.axis_size("w") + other_w
            order.append(lax.dynamic_slice_in_dim(prefix_embed, source * share, share, 0))
    embed_rows = jnp.concatenate(order, 0)
    grad_w_hidden = dot_tn(embed_rows, pre_rounded)
    grad_b_hidden = jnp.sum(pre_rounded.astype(F32), axis=0)
    return (query_grad, grad_w_out, grad_w_hidden, grad_b_hidden, grad_prefix)


def solution(mesh):
    torus = Mesh(mesh.devices.reshape(2, 8, 2, 4, 2), ("y", "z", "c", "x", "w"))
    placed = (
        P(),
        P(None, SEQ),
        P(SEQ),
        P(SEQ, None, HEAD),
        P(SEQ, HEAD),
        P(SEQ, HEAD),
        P(SEQ, HEAD),
        P(SEQ, HEAD),
    )
    return jax.shard_map(
        on_device,
        mesh=torus,
        in_specs=placed,
        out_specs=(P(SEQ, HEAD), P(SEQ, None, HEAD), P(None, SEQ), P(SEQ), P()),
        check_vma=False,
    )
```

```python
import functools
import math

import jax
import jax.numpy as jnp
from jax import lax
from jax.experimental import pallas as pl
from jax.experimental.pallas import tpu as pltpu
from jax.sharding import Mesh
from jax.sharding import PartitionSpec as P

HD = 128
SCALE = 1.0 / math.sqrt(HD)
C1 = SCALE * math.log2(math.e)
NEG = -1e30
TILE = 256
PIECES = 4
SEQ = ("y", "z", "c")
YZ = ("y", "z")
CYZ = ("c", "y", "z")
HEAD = ("x", "w")
OWNERS = ("x", "w", "y", "z")
F32 = jnp.float32
BF16 = jnp.bfloat16
SMEM = pl.BlockSpec(memory_space=pltpu.SMEM)
VMEM = pl.BlockSpec(memory_space=pltpu.VMEM)


def dot_nt(a, b):
    return lax.dot_general(a, b, (((1,), (1,)), ((), ())), preferred_element_type=F32)


def dot_nn(a, b):
    return lax.dot_general(a, b, (((1,), (0,)), ((), ())), preferred_element_type=F32)


def dot_tn(a, b):
    return lax.dot_general(a, b, (((0,), (0,)), ((), ())), preferred_element_type=F32)


def span(r):
    return slice(r * TILE, (r + 1) * TILE)


def update(state, s, d):
    m, l, t = state
    s = s.reshape(-1, 8, TILE)
    d = d.reshape(-1, 8, TILE)
    new = jnp.maximum(m, jnp.max(s, axis=0))
    fade = jnp.exp2(m - new)
    w = jnp.exp2(s - new[None])
    return (new, l * fade + jnp.sum(w, axis=0), t * fade + jnp.sum(w * d, axis=0))


def pair_of(kv, j):
    k = jnp.concatenate([kv[2 * j, :HD], kv[2 * j + 1, :HD]], 0)
    v = jnp.concatenate([kv[2 * j, HD : 2 * HD], kv[2 * j + 1, HD : 2 * HD]], 0)
    return k, v


def visible(pos, own, j, shape, key_dim):
    key = lax.broadcasted_iota(jnp.int32, shape, key_dim)
    row = lax.broadcasted_iota(jnp.int32, shape, 1 - key_dim) % HD
    if own:
        return key <= (pos[0] - 2 * j) * HD + row
    return key < (pos[0] + pos[1] - 2 * j) * HD


def sweep_kernel(pos, q, g, mine, other, out):
    tiles = q.shape[0] // TILE

    def step(j, states, masked=False):
        for own, kv in ((True, mine), (False, other)):
            k, v = pair_of(kv, j)
            seen = visible(pos, own, j, (2 * HD, TILE), 0) if masked else None
            new = []
            for r in range(tiles):
                s = dot_nt(k, q[span(r), :]) * C1
                if masked:
                    s = jnp.where(seen, s, NEG)
                new.append(update(states[r], s, dot_nt(v, g[span(r), :])))
            states = tuple(new)
        return states

    zero = jnp.zeros((8, TILE), F32)
    states = tuple((jnp.full((8, TILE), NEG, F32), zero, zero) for _ in range(tiles))
    half = pos[0] // 2
    states = step(half, lax.fori_loop(0, half, step, states), True)
    for r in range(tiles):
        for a in range(3):
            out[a, :, span(r)] = states[r][a]


def prefix_kernel(q, g, pkv, state, grads, stats):
    npre = pkv.shape[1]
    kg = jnp.zeros((npre, HD), F32)
    vg = jnp.zeros((npre, HD), F32)
    for r in range(q.shape[0] // TILE):
        s = dot_nt(pkv[0], q[span(r), :]) * C1
        d = dot_nt(pkv[1], g[span(r), :])
        m, l, t = update(tuple(state[a, :, span(r)] for a in range(3)), s, d)
        top = jnp.max(m, axis=0, keepdims=True)
        fade = jnp.exp2(m - top)
        total = jnp.sum(l * fade, axis=0, keepdims=True)
        delta = jnp.sum(t * fade, axis=0, keepdims=True) / total
        log_total = top + jnp.log2(total)
        stats[0:1, span(r)] = log_total
        stats[1:2, span(r)] = delta
        p = jnp.exp2(s - log_total)
        kg = kg + dot_nn((p * (d - delta)).astype(BF16), q[span(r), :])
        vg = vg + dot_nn(p.astype(BF16), g[span(r), :])
    grads[0] = (kg * SCALE).astype(grads.dtype)
    grads[1] = vg.astype(grads.dtype)


def grad_kernel(piece, pos, q, g, stats, mine, other, extra, out, total, log_total, delta):
    rows = q.shape[0]
    columns = stats[...].T
    log_total[...] = jnp.broadcast_to(columns[:, 0:1], (rows, HD))
    delta[...] = jnp.broadcast_to(columns[:, 1:2], (rows, HD))

    def part(k, v, seen=None):
        for r in range(rows // TILE):
            s = dot_nt(q[span(r), :], k) * C1
            if seen is not None:
                s = jnp.where(seen, s, NEG)
            d = dot_nt(g[span(r), :], v)
            pieces = []
            for b in range(k.shape[0] // HD):
                lanes = slice(b * HD, (b + 1) * HD)
                p = jnp.exp2(s[:, lanes] - log_total[span(r), :])
                pieces.append((p * (d[:, lanes] - delta[span(r), :])).astype(BF16))
            total[span(r), :] += dot_nn(jnp.concatenate(pieces, 1), k)

    def step(i, masked=False):
        for own, kv in ((True, mine), (False, other)):
            k, v = pair_of(kv, i)
            seen = visible(pos, own, first + i, (TILE, 2 * HD), 1) if masked else None
            part(k, v, seen)

    if piece == 0:
        total[...] = jnp.zeros((rows, HD), F32)
        part(extra[0], extra[1])
    else:
        total[...] = extra[...]
    pairs = mine.shape[0] // 2
    first = piece * pairs
    half = pos[0] // 2
    lax.fori_loop(0, jnp.clip(half - first, 0, pairs), lambda i, _: step(i), None)

    @pl.when((half >= first) & (half < first + pairs))
    def _():
        step(half - first, True)

    if piece < PIECES - 1:
        out[...] = total[...]
    else:
        result = (total[...] * SCALE).astype(out.dtype)
        for h in range(rows // HD):
            out[:, h * HD : (h + 1) * HD] = result[h * HD : (h + 1) * HD]


def sweep(pos, q, g, mine, other):
    return pl.pallas_call(
        sweep_kernel,
        out_shape=jax.ShapeDtypeStruct((3, 8, q.shape[0]), F32),
        in_specs=[SMEM] + [VMEM] * 4,
        out_specs=VMEM,
        cost_estimate=pl.CostEstimate(flops=2 * 10**9, bytes_accessed=3 * 10**6, transcendentals=4 * 10**6),
        name="sweep",
    )(pos, q, g, mine, other)


def prefix_part(q, g, pkv, state):
    return pl.pallas_call(
        prefix_kernel,
        out_shape=(
            jax.ShapeDtypeStruct(pkv.shape, BF16),
            jax.ShapeDtypeStruct((2, q.shape[0]), F32),
        ),
        in_specs=[VMEM] * 4,
        out_specs=(VMEM, VMEM),
        cost_estimate=pl.CostEstimate(flops=3 * 10**8, bytes_accessed=10**6, transcendentals=5 * 10**5),
        name="prefix_part",
    )(q, g, pkv, state)


def whole(value):
    return pl.BlockSpec(value.shape, lambda *_: (0,) * value.ndim)


def query_grad_piece(piece, pos, q, g, stats, mine, other, extra):
    n = q.shape[0]
    blocks, *shape = mine.shape
    part = pl.BlockSpec((blocks // PIECES, *shape), lambda *_: (piece, 0, 0))
    out = jax.ShapeDtypeStruct((n, HD), F32)
    if piece == PIECES - 1:
        out = jax.ShapeDtypeStruct((HD, n), BF16)
    return pl.pallas_call(
        functools.partial(grad_kernel, piece),
        out_shape=out,
        in_specs=[SMEM, whole(q), whole(g), whole(stats), part, part, whole(extra)],
        out_specs=whole(out),
        grid=(1,),
        scratch_shapes=[pltpu.VMEM((n, HD), F32)] * 3,
        cost_estimate=pl.CostEstimate(flops=10**9, bytes_accessed=3 * 10**6, transcendentals=10**6),
        name="query_grad",
    )(pos, q, g, stats, mine, other, extra)


def w_hidden_kernel(place, embed, *refs):
    *parts, grad_w, grad_b, pre = refs
    lines = len(parts)
    share = parts[0].shape[0] // 2
    for k, part in enumerate(parts):
        line = (place[0] + lines - k) % lines
        for side in range(2):
            source = 2 * line + (place[1] + side) % 2
            pre[pl.ds(pl.multiple_of(source * share, share), share), :] = part[side * share : (side + 1) * share]
    grad_w[...] = dot_tn(embed[...], pre[...])
    grad_b[...] = jnp.sum(pre[...].astype(F32), axis=0)


def w_hidden_grad(place, embed, *parts):
    npre, emb = embed.shape
    units = parts[0].shape[1]
    return pl.pallas_call(
        w_hidden_kernel,
        out_shape=(jax.ShapeDtypeStruct((emb, units), F32), jax.ShapeDtypeStruct((units,), F32)),
        in_specs=[SMEM] + [VMEM] * (1 + len(parts)),
        out_specs=(VMEM, VMEM),
        scratch_shapes=[pltpu.VMEM((npre, units), BF16)],
        cost_estimate=pl.CostEstimate(flops=2 * 10**8, bytes_accessed=2 * 10**6, transcendentals=0),
        name="w_hidden_grad",
    )(place, embed, *parts)


def exchange(value, axes):
    return lax.all_to_all(value, axes, 0, 0, tiled=True)


def to_all(value, axes):
    return exchange(jnp.broadcast_to(value, (lax.axis_size(axes), *value.shape)), axes)


def sum_parts(value, axes, dtype=BF16):
    parts = exchange(value.reshape(lax.axis_size(axes), -1, HD).astype(dtype), axes)
    return jnp.sum(parts.astype(F32), axis=0)


def shift(value, axis, steps):
    count = lax.axis_size(axis)
    return lax.ppermute(value, axis, [(i, (i + steps) % count) for i in range(count)])


def by_head(rows):
    return rows.reshape(rows.shape[0], -1, HD).transpose(1, 0, 2).reshape(-1, HD)


def on_device(prefix_embed, w_hidden, b_hidden, w_out, queries, keys, values, out_grad):
    npre, emb = prefix_embed.shape
    units = w_hidden.shape[1]
    core = lax.axis_index("c")
    here = lax.axis_index(YZ)
    head = lax.axis_index(HEAD)
    heads = lax.axis_size(HEAD)
    share = npre // heads
    pos = jnp.stack([here, core]).astype(jnp.int32)

    hidden_pre = jnp.dot(prefix_embed, w_hidden, preferred_element_type=F32) + b_hidden
    tangent = jnp.tanh(hidden_pre)
    hidden = tangent.astype(BF16)
    partial_kv = jnp.einsum("ph,hck->cpk", hidden, w_out, preferred_element_type=F32)
    groups = lax.axis_size(YZ)
    kv = jnp.concatenate([keys, values], 0)
    partial_kv = partial_kv.reshape(groups, -1, HD).astype(BF16)
    mine = exchange(jnp.concatenate([jnp.broadcast_to(kv, (groups, *kv.shape)), partial_kv], 1), YZ)
    own = jnp.sum(mine[:, kv.shape[0] :].astype(F32), axis=0)
    own = (own + shift(own, "c", 1)).astype(BF16)
    other = shift(mine, "c", 1)
    pkv = to_all(own, YZ).reshape(2, npre, HD)
    q = by_head(queries)
    g = by_head(out_grad)
    state = sweep(pos, q, g, mine, other)
    grads, stats = prefix_part(q, g, pkv, state)
    own_grads = sum_parts(grads, SEQ).astype(BF16)
    prefix_grads = to_all(own_grads, SEQ).reshape(2, npre, HD)
    query_grad = pkv
    for piece in range(PIECES):
        query_grad = query_grad_piece(piece, pos, q, g, stats, mine, other, query_grad)
    grad_w_out = jnp.einsum("ph,cpk->hck", hidden, prefix_grads, preferred_element_type=F32)
    hidden_part = jnp.einsum("cpk,hck->ph", prefix_grads, w_out, preferred_element_type=F32)
    parts = exchange(hidden_part.reshape(heads, share, units), HEAD)
    hidden_grad = jnp.sum(parts, axis=0)
    own_tangent = lax.dynamic_slice_in_dim(tangent, head * share, share, 0)
    pre_part = (hidden_grad * (1.0 - own_tangent * own_tangent)).astype(BF16)
    embed_part = dot_nt(pre_part, w_hidden)
    own_embed = sum_parts(embed_part, CYZ).astype(BF16)
    near = to_all(own_embed, OWNERS)
    far = shift(near, "c", 1)
    sides = jnp.stack([jnp.where(core == 0, near, far), jnp.where(core == 0, far, near)], 0)
    sides = sides.reshape(2, heads, -1, emb).transpose(1, 0, 2, 3)
    grad_prefix = sides.reshape(npre, emb).astype(F32)
    both = jnp.concatenate([pre_part, shift(pre_part, "w", 1)], 0)
    turns = [shift(both, "x", k) for k in range(1, lax.axis_size("x"))]
    place = jnp.stack([lax.axis_index("x"), lax.axis_index("w")]).astype(jnp.int32)
    grad_w_hidden, grad_b_hidden = w_hidden_grad(place, prefix_embed, both, *turns)
    return (query_grad, grad_w_out, grad_w_hidden, grad_b_hidden, grad_prefix)


def solution(mesh):
    torus = Mesh(mesh.devices.reshape(2, 8, 2, 4, 2), ("y", "z", "c", "x", "w"))
    placed = (
        P(),
        P(None, SEQ),
        P(SEQ),
        P(SEQ, None, HEAD),
        P(SEQ, HEAD),
        P(SEQ, HEAD),
        P(SEQ, HEAD),
        P(SEQ, HEAD),
    )
    return jax.shard_map(
        on_device,
        mesh=torus,
        in_specs=placed,
        out_specs=(P(SEQ, HEAD), P(SEQ, None, HEAD), P(None, SEQ), P(SEQ), P()),
        check_vma=False,
    )
```

```python
import functools
import math

import jax
import jax.numpy as jnp
from jax import lax
from jax.experimental import pallas as pl
from jax.experimental.pallas import tpu as pltpu
from jax.sharding import Mesh
from jax.sharding import PartitionSpec as P

HD = 128
SCALE = 1.0 / math.sqrt(HD)
C1 = SCALE * math.log2(math.e)
NEG = -1e30
TILE = 256
PIECES = 2
SEQ = ("y", "z", "c")
CYZ = ("c", "y", "z")
HEAD = ("x", "w")
OWNERS = ("x", "w", "y", "z")
F32 = jnp.float32
BF16 = jnp.bfloat16
SMEM = pl.BlockSpec(memory_space=pltpu.SMEM)
VMEM = pl.BlockSpec(memory_space=pltpu.VMEM)


def dot_nt(a, b):
    return lax.dot_general(a, b, (((1,), (1,)), ((), ())), preferred_element_type=F32)


def dot_nn(a, b):
    return lax.dot_general(a, b, (((1,), (0,)), ((), ())), preferred_element_type=F32)


def dot_tn(a, b):
    return lax.dot_general(a, b, (((0,), (0,)), ((), ())), preferred_element_type=F32)


def span(r):
    return slice(r * TILE, (r + 1) * TILE)


def update(state, s, d):
    m, l, t = state
    s = s.reshape(-1, 8, TILE)
    d = d.reshape(-1, 8, TILE)
    new = jnp.maximum(m, jnp.max(s, axis=0))
    fade = jnp.exp2(m - new)
    w = jnp.exp2(s - new[None])
    return (new, l * fade + jnp.sum(w, axis=0), t * fade + jnp.sum(w * d, axis=0))


def pair_of(kv, j):
    k = jnp.concatenate([kv[2 * j, :HD], kv[2 * j + 1, :HD]], 0)
    v = jnp.concatenate([kv[2 * j, HD : 2 * HD], kv[2 * j + 1, HD : 2 * HD]], 0)
    return k, v


def visible(pos, own, j, shape, key_dim):
    key = lax.broadcasted_iota(jnp.int32, shape, key_dim)
    row = lax.broadcasted_iota(jnp.int32, shape, 1 - key_dim) % HD
    if own:
        return key <= (pos[0] - 2 * j) * HD + row
    return key < (pos[0] + pos[1] - 2 * j) * HD


def sweep_step(pos, q, g, mine, other, j, states, masked=False):
    for own, kv in ((True, mine), (False, other)):
        k, v = pair_of(kv, j)
        seen = visible(pos, own, j, (2 * HD, TILE), 0) if masked else None
        new = []
        for r in range(q.shape[0] // TILE):
            s = dot_nt(k, q[span(r), :]) * C1
            if masked:
                s = jnp.where(seen, s, NEG)
            new.append(update(states[r], s, dot_nt(v, g[span(r), :])))
        states = tuple(new)
    return states


def empty_states(tiles):
    zero = jnp.zeros((8, TILE), F32)
    return tuple((jnp.full((8, TILE), NEG, F32), zero, zero) for _ in range(tiles))


def sweep_kernel(pos, q, g, mine, other, out):
    tiles = q.shape[0] // TILE
    step = functools.partial(sweep_step, pos, q, g, mine, other)
    half = pos[0] // 2
    states = step(half, lax.fori_loop(0, half, step, empty_states(tiles)), True)
    for r in range(tiles):
        for a in range(3):
            out[a, :, span(r)] = states[r][a]


def merged(m, l, t):
    top = jnp.max(m, axis=0, keepdims=True)
    fade = jnp.exp2(m - top)
    return top, jnp.sum(l * fade, axis=0, keepdims=True), jnp.sum(t * fade, axis=0, keepdims=True)


def lent_sweep_kernel(pos, q, g, mine, other, out):
    tiles = q.shape[0] // TILE
    step = functools.partial(sweep_step, pos, q, g, mine, other)
    pairs = jnp.where(pos[2] == 0, mine.shape[0] // 2, 0)
    states = lax.fori_loop(0, pairs, step, empty_states(tiles))
    for r in range(tiles):
        for a, value in enumerate(merged(*states[r])):
            out[a : a + 1, span(r)] = value


def prefix_kernel(pos, q, g, pkv, state, lent, grads, stats):
    npre = pkv.shape[1]
    kg = jnp.zeros((npre, HD), F32)
    vg = jnp.zeros((npre, HD), F32)
    late = pos[2] == 1
    for r in range(q.shape[0] // TILE):
        s = dot_nt(pkv[0], q[span(r), :]) * C1
        d = dot_nt(pkv[1], g[span(r), :])
        near = merged(*update(tuple(state[a, :, span(r)] for a in range(3)), s, d))
        far = tuple(
            jnp.where(late, lent[a : a + 1, span(r)], empty) for a, empty in enumerate((NEG, 0.0, 0.0))
        )
        top = jnp.maximum(near[0], far[0])
        near_fade = jnp.exp2(near[0] - top)
        far_fade = jnp.exp2(far[0] - top)
        total = near[1] * near_fade + far[1] * far_fade
        delta = (near[2] * near_fade + far[2] * far_fade) / total
        log_total = top + jnp.log2(total)
        stats[0:1, span(r)] = log_total
        stats[1:2, span(r)] = delta
        p = jnp.exp2(s - log_total)
        kg = kg + dot_nn((p * (d - delta)).astype(BF16), q[span(r), :])
        vg = vg + dot_nn(p.astype(BF16), g[span(r), :])
    grads[0] = (kg * SCALE).astype(grads.dtype)
    grads[1] = vg.astype(grads.dtype)


def grad_kernel(lent, piece, pos, q, g, stats, mine, other, *refs):
    *extra, out, total, log_total, delta = refs
    rows = q.shape[0]
    pairs = mine.shape[0] // 2
    first = piece * pairs

    def part(k, v, seen=None):
        for r in range(rows // TILE):
            s = dot_nt(q[span(r), :], k) * C1
            if seen is not None:
                s = jnp.where(seen, s, NEG)
            d = dot_nt(g[span(r), :], v)
            pieces = []
            for b in range(k.shape[0] // HD):
                lanes = slice(b * HD, (b + 1) * HD)
                p = jnp.exp2(s[:, lanes] - log_total[span(r), :])
                pieces.append((p * (d[:, lanes] - delta[span(r), :])).astype(BF16))
            total[span(r), :] += dot_nn(jnp.concatenate(pieces, 1), k)

    def step(i, masked=False):
        for own, kv in ((True, mine), (False, other)):
            k, v = pair_of(kv, i)
            seen = visible(pos, own, first + i, (TILE, 2 * HD), 1) if masked else None
            part(k, v, seen)

    def spread():
        columns = stats[...].T
        log_total[...] = jnp.broadcast_to(columns[:, 0:1], (rows, HD))
        delta[...] = jnp.broadcast_to(columns[:, 1:2], (rows, HD))

    if piece == 0:
        total[...] = jnp.zeros((rows, HD), F32)
    else:
        total[...] = extra[0][...]
    if lent:

        @pl.when(pos[2] == 0)
        def _():
            spread()
            lax.fori_loop(0, pairs, lambda i, _: step(i), None)

    else:
        spread()
        if piece == 0:
            part(extra[0][0], extra[0][1])
        half = pos[0] // 2
        lax.fori_loop(0, jnp.clip(half - first, 0, pairs), lambda i, _: step(i), None)

        @pl.when((half >= first) & (half < first + pairs))
        def _():
            step(half - first, True)

    if piece < PIECES - 1:
        out[...] = total[...]
    else:
        out[...] = (total[...] * SCALE).astype(out.dtype)


def sweep(pos, q, g, mine, other):
    return pl.pallas_call(
        sweep_kernel,
        out_shape=jax.ShapeDtypeStruct((3, 8, q.shape[0]), F32),
        in_specs=[SMEM] + [VMEM] * 4,
        out_specs=VMEM,
        cost_estimate=pl.CostEstimate(flops=10**9, bytes_accessed=2 * 10**6, transcendentals=2 * 10**6),
        name="sweep",
    )(pos, q, g, mine, other)


def lent_sweep(pos, q, g, mine, other):
    return pl.pallas_call(
        lent_sweep_kernel,
        out_shape=jax.ShapeDtypeStruct((3, q.shape[0]), F32),
        in_specs=[SMEM] + [VMEM] * 4,
        out_specs=VMEM,
        cost_estimate=pl.CostEstimate(flops=10**9, bytes_accessed=2 * 10**6, transcendentals=2 * 10**6),
        name="lent_sweep",
    )(pos, q, g, mine, other)


def prefix_part(pos, q, g, pkv, state, lent):
    return pl.pallas_call(
        prefix_kernel,
        out_shape=(
            jax.ShapeDtypeStruct(pkv.shape, BF16),
            jax.ShapeDtypeStruct((2, q.shape[0]), F32),
        ),
        in_specs=[SMEM] + [VMEM] * 5,
        out_specs=(VMEM, VMEM),
        cost_estimate=pl.CostEstimate(flops=3 * 10**8, bytes_accessed=10**6, transcendentals=5 * 10**5),
        name="prefix_part",
    )(pos, q, g, pkv, state, lent)


def whole(value):
    return pl.BlockSpec(value.shape, lambda *_: (0,) * value.ndim)


def query_grad_piece(lent, piece, pos, q, g, stats, mine, other, *extra):
    blocks, *shape = mine.shape
    part = pl.BlockSpec((blocks // PIECES, *shape), lambda *_: (piece, 0, 0))
    out = jax.ShapeDtypeStruct(q.shape, BF16 if lent and piece == PIECES - 1 else F32)
    return pl.pallas_call(
        functools.partial(grad_kernel, lent, piece),
        out_shape=out,
        in_specs=[SMEM, whole(q), whole(g), whole(stats), part, part] + [whole(v) for v in extra],
        out_specs=whole(out),
        grid=(1,),
        scratch_shapes=[pltpu.VMEM(q.shape, F32)] * 3,
        cost_estimate=pl.CostEstimate(flops=10**9, bytes_accessed=3 * 10**6, transcendentals=10**6),
        name="query_grad",
    )(pos, q, g, stats, mine, other, *extra)


def w_hidden_kernel(place, embed, *refs):
    *parts, grad_w, grad_b, pre = refs
    lines = len(parts)
    share = parts[0].shape[0] // 2
    for k, part in enumerate(parts):
        line = (place[0] + lines - k) % lines
        for side in range(2):
            source = 2 * line + (place[1] + side) % 2
            pre[pl.ds(pl.multiple_of(source * share, share), share), :] = part[side * share : (side + 1) * share]
    grad_w[...] = dot_tn(embed[...], pre[...])
    grad_b[...] = jnp.sum(pre[...].astype(F32), axis=0)


def w_hidden_grad(place, embed, *parts):
    npre, emb = embed.shape
    units = parts[0].shape[1]
    return pl.pallas_call(
        w_hidden_kernel,
        out_shape=(jax.ShapeDtypeStruct((emb, units), F32), jax.ShapeDtypeStruct((units,), F32)),
        in_specs=[SMEM] + [VMEM] * (1 + len(parts)),
        out_specs=(VMEM, VMEM),
        scratch_shapes=[pltpu.VMEM((npre, units), BF16)],
        cost_estimate=pl.CostEstimate(flops=2 * 10**8, bytes_accessed=2 * 10**6, transcendentals=0),
        name="w_hidden_grad",
    )(place, embed, *parts)


def exchange(value, axes):
    return lax.all_to_all(value, axes, 0, 0, tiled=True)


def to_all(value, axes):
    return exchange(jnp.broadcast_to(value, (lax.axis_size(axes), *value.shape)), axes)


def sum_parts(value, axes, dtype=BF16):
    parts = exchange(value.reshape(lax.axis_size(axes), -1, HD).astype(dtype), axes)
    return jnp.sum(parts.astype(F32), axis=0)


def shift(value, axis, steps):
    count = lax.axis_size(axis)
    return lax.ppermute(value, axis, [(i, (i + steps) % count) for i in range(count)])


def by_head(rows):
    return rows.reshape(rows.shape[0], -1, HD).transpose(1, 0, 2).reshape(-1, HD)


def on_device(prefix_embed, w_hidden, b_hidden, w_out, queries, keys, values, out_grad):
    npre, emb = prefix_embed.shape
    units = w_hidden.shape[1]
    core = lax.axis_index("c")
    late = lax.axis_index("y")
    head = lax.axis_index(HEAD)
    heads = lax.axis_size(HEAD)
    share = npre // heads
    pos = jnp.stack([lax.axis_index("z"), core, late]).astype(jnp.int32)

    hidden_pre = jnp.dot(prefix_embed, w_hidden, preferred_element_type=F32) + b_hidden
    tangent = jnp.tanh(hidden_pre)
    hidden = tangent.astype(BF16)
    partial_kv = jnp.einsum("ph,hck->cpk", hidden, w_out, preferred_element_type=F32)
    groups = lax.axis_size("z")
    kv = jnp.concatenate([keys, values], 0)
    partial_kv = partial_kv.reshape(groups, -1, HD).astype(BF16)
    mine = exchange(
        jnp.concatenate([jnp.broadcast_to(kv, (groups, *kv.shape)), partial_kv], 1), "z"
    )
    q = by_head(queries)
    g = by_head(out_grad)
    lent_q = lax.ppermute(queries, "y", [(1, 0)])
    lent_g = lax.ppermute(out_grad, "y", [(1, 0)])
    lent_q = by_head(lent_q)
    lent_g = by_head(lent_g)
    other = shift(mine, "c", 1)
    own = jnp.sum(mine[:, kv.shape[0] :].astype(F32), axis=0)
    own = own + shift(own, "c", 1)
    own = (own + shift(own, "y", 1)).astype(BF16)
    pkv = to_all(own, "z").reshape(2, npre, HD)
    lent_state = lent_sweep(pos, lent_q, lent_g, mine, other)
    lent_state = lax.ppermute(lent_state, "y", [(0, 1)])
    state = sweep(pos, q, g, mine, other)
    grads, stats = prefix_part(pos, q, g, pkv, state, lent_state)
    lent_stats = lax.ppermute(stats, "y", [(1, 0)])
    own_grads = sum_parts(grads, SEQ).astype(BF16)
    prefix_grads = to_all(own_grads, SEQ).reshape(2, npre, HD)
    lent_grad = ()
    for piece in range(PIECES):
        lent_grad = (
            query_grad_piece(True, piece, pos, lent_q, lent_g, lent_stats, mine, other, *lent_grad),
        )
    lent_grad = lax.ppermute(*lent_grad, "y", [(0, 1)])
    query_grad = pkv
    for piece in range(PIECES):
        query_grad = query_grad_piece(False, piece, pos, q, g, stats, mine, other, query_grad)
    query_grad = (query_grad + lent_grad.astype(F32)).astype(BF16)
    query_grad = query_grad.reshape(-1, queries.shape[0], HD).transpose(1, 0, 2).reshape(queries.shape)
    grad_w_out = jnp.einsum("ph,cpk->hck", hidden, prefix_grads, preferred_element_type=F32)
    hidden_part = jnp.einsum("cpk,hck->ph", prefix_grads, w_out, preferred_element_type=F32)
    parts = exchange(hidden_part.reshape(heads, share, units), HEAD)
    hidden_grad = jnp.sum(parts, axis=0)
    own_tangent = lax.dynamic_slice_in_dim(tangent, head * share, share, 0)
    pre_part = (hidden_grad * (1.0 - own_tangent * own_tangent)).astype(BF16)
    embed_part = dot_nt(pre_part, w_hidden)
    own_embed = sum_parts(embed_part, CYZ).astype(BF16)
    near = to_all(own_embed, OWNERS)
    far = shift(near, "c", 1)
    sides = jnp.stack([jnp.where(core == 0, near, far), jnp.where(core == 0, far, near)], 0)
    sides = sides.reshape(2, heads, -1, emb).transpose(1, 0, 2, 3)
    grad_prefix = sides.reshape(npre, emb).astype(F32)
    both = jnp.concatenate([pre_part, shift(pre_part, "w", 1)], 0)
    turns = [shift(both, "x", k) for k in range(1, lax.axis_size("x"))]
    place = jnp.stack([lax.axis_index("x"), lax.axis_index("w")]).astype(jnp.int32)
    grad_w_hidden, grad_b_hidden = w_hidden_grad(place, prefix_embed, both, *turns)
    return (query_grad, grad_w_out, grad_w_hidden, grad_b_hidden, grad_prefix)


def solution(mesh):
    torus = Mesh(mesh.devices.reshape(2, 8, 2, 4, 2), ("y", "z", "c", "x", "w"))
    placed = (
        P(),
        P(None, SEQ),
        P(SEQ),
        P(SEQ, None, HEAD),
        P(SEQ, HEAD),
        P(SEQ, HEAD),
        P(SEQ, HEAD),
        P(SEQ, HEAD),
    )
    return jax.shard_map(
        on_device,
        mesh=torus,
        in_specs=placed,
        out_specs=(P(SEQ, HEAD), P(SEQ, None, HEAD), P(None, SEQ), P(SEQ), P()),
        check_vma=False,
    )
```

```python
import functools
import math

import jax
import jax.numpy as jnp
from jax import lax
from jax.experimental import pallas as pl
from jax.experimental.pallas import tpu as pltpu
from jax.sharding import Mesh
from jax.sharding import PartitionSpec as P

HD = 128
SCALE = 1.0 / math.sqrt(HD)
C1 = SCALE * math.log2(math.e)
NEG = -1e30
TILE = 256
PIECES = 2
SEQ = ("y", "z", "c")
CYZ = ("c", "y", "z")
HEAD = ("x", "w")
OWNERS = ("x", "w", "y", "z")
F32 = jnp.float32
BF16 = jnp.bfloat16
SMEM = pl.BlockSpec(memory_space=pltpu.SMEM)
VMEM = pl.BlockSpec(memory_space=pltpu.VMEM)


def dot_nt(a, b):
    return lax.dot_general(a, b, (((1,), (1,)), ((), ())), preferred_element_type=F32)


def dot_nn(a, b):
    return lax.dot_general(a, b, (((1,), (0,)), ((), ())), preferred_element_type=F32)


def dot_tn(a, b):
    return lax.dot_general(a, b, (((0,), (0,)), ((), ())), preferred_element_type=F32)


def span(r):
    return slice(r * TILE, (r + 1) * TILE)


def update(state, s, d):
    m, l, t = state
    s = s.reshape(-1, 8, TILE)
    d = d.reshape(-1, 8, TILE)
    new = jnp.maximum(m, jnp.max(s, axis=0))
    fade = jnp.exp2(m - new)
    w = jnp.exp2(s - new[None])
    return (new, l * fade + jnp.sum(w, axis=0), t * fade + jnp.sum(w * d, axis=0))


def pair_of(kv, j):
    k = jnp.concatenate([kv[2 * j, :HD], kv[2 * j + 1, :HD]], 0)
    v = jnp.concatenate([kv[2 * j, HD : 2 * HD], kv[2 * j + 1, HD : 2 * HD]], 0)
    return k, v


def visible(pos, own, j, shape, key_dim):
    key = lax.broadcasted_iota(jnp.int32, shape, key_dim)
    row = lax.broadcasted_iota(jnp.int32, shape, 1 - key_dim) % HD
    if own:
        return key <= (pos[0] - 2 * j) * HD + row
    return key < (pos[0] + pos[1] - 2 * j) * HD


def sweep_step(pos, q, g, mine, other, j, states, masked=False):
    for own, kv in ((True, mine), (False, other)):
        k, v = pair_of(kv, j)
        seen = visible(pos, own, j, (2 * HD, TILE), 0) if masked else None
        new = []
        for r in range(q.shape[0] // TILE):
            s = dot_nt(k, q[span(r), :]) * C1
            if masked:
                s = jnp.where(seen, s, NEG)
            new.append(update(states[r], s, dot_nt(v, g[span(r), :])))
        states = tuple(new)
    return states


def empty_states(tiles):
    zero = jnp.zeros((8, TILE), F32)
    return tuple((jnp.full((8, TILE), NEG, F32), zero, zero) for _ in range(tiles))


def sweep_kernel(pos, q, g, mine, other, out):
    tiles = q.shape[0] // TILE
    step = functools.partial(sweep_step, pos, q, g, mine, other)
    half = pos[0] // 2
    states = step(half, lax.fori_loop(0, half, step, empty_states(tiles)), True)
    for r in range(tiles):
        for a in range(3):
            out[a, :, span(r)] = states[r][a]


def merged(m, l, t):
    top = jnp.max(m, axis=0, keepdims=True)
    fade = jnp.exp2(m - top)
    return top, jnp.sum(l * fade, axis=0, keepdims=True), jnp.sum(t * fade, axis=0, keepdims=True)


def lent_sweep_kernel(pos, q, g, mine, other, out):
    tiles = q.shape[0] // TILE
    step = functools.partial(sweep_step, pos, q, g, mine, other)
    pairs = jnp.where(pos[2] == 0, mine.shape[0] // 2, 0)
    states = lax.fori_loop(0, pairs, step, empty_states(tiles))
    for r in range(tiles):
        for a, value in enumerate(merged(*states[r])):
            out[a : a + 1, span(r)] = value


def prefix_kernel(pos, q, g, pkv, state, lent, grads, stats):
    npre = pkv.shape[1]
    kg = jnp.zeros((npre, HD), F32)
    vg = jnp.zeros((npre, HD), F32)
    late = pos[2] == 1
    for r in range(q.shape[0] // TILE):
        s = dot_nt(pkv[0], q[span(r), :]) * C1
        d = dot_nt(pkv[1], g[span(r), :])
        near = merged(*update(tuple(state[a, :, span(r)] for a in range(3)), s, d))
        far = tuple(
            jnp.where(late, lent[a : a + 1, span(r)], empty) for a, empty in enumerate((NEG, 0.0, 0.0))
        )
        top = jnp.maximum(near[0], far[0])
        near_fade = jnp.exp2(near[0] - top)
        far_fade = jnp.exp2(far[0] - top)
        total = near[1] * near_fade + far[1] * far_fade
        delta = (near[2] * near_fade + far[2] * far_fade) / total
        log_total = top + jnp.log2(total)
        stats[0:1, span(r)] = log_total
        stats[1:2, span(r)] = delta
        p = jnp.exp2(s - log_total)
        kg = kg + dot_nn((p * (d - delta)).astype(BF16), q[span(r), :])
        vg = vg + dot_nn(p.astype(BF16), g[span(r), :])
    grads[0] = (kg * SCALE).astype(grads.dtype)
    grads[1] = vg.astype(grads.dtype)


def grad_kernel(lent, piece, pos, q, g, stats, mine, other, *refs):
    *extra, out, total, log_total, delta = refs
    rows = q.shape[0]
    pairs = mine.shape[0] // 2
    first = piece * pairs

    def part(k, v, seen=None):
        for r in range(rows // TILE):
            s = dot_nt(q[span(r), :], k) * C1
            if seen is not None:
                s = jnp.where(seen, s, NEG)
            d = dot_nt(g[span(r), :], v)
            pieces = []
            for b in range(k.shape[0] // HD):
                lanes = slice(b * HD, (b + 1) * HD)
                p = jnp.exp2(s[:, lanes] - log_total[span(r), :])
                pieces.append((p * (d[:, lanes] - delta[span(r), :])).astype(BF16))
            total[span(r), :] += dot_nn(jnp.concatenate(pieces, 1), k)

    def step(i, masked=False):
        for own, kv in ((True, mine), (False, other)):
            k, v = pair_of(kv, i)
            seen = visible(pos, own, first + i, (TILE, 2 * HD), 1) if masked else None
            part(k, v, seen)

    def spread():
        columns = stats[...].T
        log_total[...] = jnp.broadcast_to(columns[:, 0:1], (rows, HD))
        delta[...] = jnp.broadcast_to(columns[:, 1:2], (rows, HD))

    if piece == 0:
        total[...] = jnp.zeros((rows, HD), F32)
    else:
        total[...] = extra[0][...]
    if lent:

        @pl.when(pos[2] == 0)
        def _():
            spread()
            lax.fori_loop(0, pairs, lambda i, _: step(i), None)

    else:
        spread()
        if piece == 0:
            part(extra[0][0], extra[0][1])
        half = pos[0] // 2
        lax.fori_loop(0, jnp.clip(half - first, 0, pairs), lambda i, _: step(i), None)

        @pl.when((half >= first) & (half < first + pairs))
        def _():
            step(half - first, True)

    if piece < PIECES - 1:
        out[...] = total[...]
    else:
        for h in range(rows // HD):
            at = slice(h * HD, (h + 1) * HD)
            out[:, at] = (total[at, :] * SCALE).astype(out.dtype)


def sweep(pos, q, g, mine, other):
    return pl.pallas_call(
        sweep_kernel,
        out_shape=jax.ShapeDtypeStruct((3, 8, q.shape[0]), F32),
        in_specs=[SMEM] + [VMEM] * 4,
        out_specs=VMEM,
        cost_estimate=pl.CostEstimate(flops=10**9, bytes_accessed=2 * 10**6, transcendentals=2 * 10**6),
        name="sweep",
    )(pos, q, g, mine, other)


def lent_sweep(pos, q, g, mine, other):
    return pl.pallas_call(
        lent_sweep_kernel,
        out_shape=jax.ShapeDtypeStruct((3, q.shape[0]), F32),
        in_specs=[SMEM] + [VMEM] * 4,
        out_specs=VMEM,
        cost_estimate=pl.CostEstimate(flops=10**9, bytes_accessed=2 * 10**6, transcendentals=2 * 10**6),
        name="lent_sweep",
    )(pos, q, g, mine, other)


def prefix_part(pos, q, g, pkv, state, lent):
    return pl.pallas_call(
        prefix_kernel,
        out_shape=(
            jax.ShapeDtypeStruct(pkv.shape, BF16),
            jax.ShapeDtypeStruct((2, q.shape[0]), F32),
        ),
        in_specs=[SMEM] + [VMEM] * 5,
        out_specs=(VMEM, VMEM),
        cost_estimate=pl.CostEstimate(flops=3 * 10**8, bytes_accessed=10**6, transcendentals=5 * 10**5),
        name="prefix_part",
    )(pos, q, g, pkv, state, lent)


def whole(value):
    return pl.BlockSpec(value.shape, lambda *_: (0,) * value.ndim)


def query_grad_piece(lent, piece, pos, q, g, stats, mine, other, *extra):
    blocks, *shape = mine.shape
    part = pl.BlockSpec((blocks // PIECES, *shape), lambda *_: (piece, 0, 0))
    out = jax.ShapeDtypeStruct(q.shape, F32)
    if piece == PIECES - 1:
        out = jax.ShapeDtypeStruct(q.shape[::-1], BF16 if lent else F32)
    return pl.pallas_call(
        functools.partial(grad_kernel, lent, piece),
        out_shape=out,
        in_specs=[SMEM, whole(q), whole(g), whole(stats), part, part] + [whole(v) for v in extra],
        out_specs=whole(out),
        grid=(1,),
        scratch_shapes=[pltpu.VMEM(q.shape, F32)] * 3,
        cost_estimate=pl.CostEstimate(flops=10**9, bytes_accessed=3 * 10**6, transcendentals=10**6),
        name="query_grad",
    )(pos, q, g, stats, mine, other, *extra)


def w_hidden_kernel(embed, pre, out):
    out[...] = dot_tn(embed[...], pre[...])


def w_hidden_grad(embed, pre):
    return pl.pallas_call(
        w_hidden_kernel,
        out_shape=jax.ShapeDtypeStruct((embed.shape[1], pre.shape[1]), F32),
        in_specs=[VMEM] * 2,
        out_specs=VMEM,
        cost_estimate=pl.CostEstimate(flops=2 * 10**8, bytes_accessed=2 * 10**6, transcendentals=0),
        name="w_hidden_grad",
    )(embed, pre)


def w_out_kernel(hidden, grads, out):
    for c in range(grads.shape[0]):
        out[:, c, :] = dot_tn(hidden[...], grads[c])


def w_out_grad(hidden, grads):
    return pl.pallas_call(
        w_out_kernel,
        out_shape=jax.ShapeDtypeStruct((hidden.shape[1], grads.shape[0], HD), F32),
        in_specs=[VMEM] * 2,
        out_specs=VMEM,
        cost_estimate=pl.CostEstimate(flops=10**8, bytes_accessed=10**6, transcendentals=0),
        name="w_out_grad",
    )(hidden, grads)


def exchange(value, axes):
    return lax.all_to_all(value, axes, 0, 0, tiled=True)


def to_all(value, axes):
    return exchange(jnp.broadcast_to(value, (lax.axis_size(axes), *value.shape)), axes)


def sum_parts(value, axes, dtype=BF16):
    parts = exchange(value.reshape(lax.axis_size(axes), -1, HD).astype(dtype), axes)
    return jnp.sum(parts.astype(F32), axis=0)


def shift(value, axis, steps):
    count = lax.axis_size(axis)
    return lax.ppermute(value, axis, [(i, (i + steps) % count) for i in range(count)])


def by_head(rows):
    return rows.reshape(rows.shape[0], -1, HD).transpose(1, 0, 2).reshape(-1, HD)


def on_device(prefix_embed, w_hidden, b_hidden, w_out, queries, keys, values, out_grad):
    npre, emb = prefix_embed.shape
    units = w_hidden.shape[1]
    core = lax.axis_index("c")
    late = lax.axis_index("y")
    head = lax.axis_index(HEAD)
    heads = lax.axis_size(HEAD)
    share = npre // heads
    pos = jnp.stack([lax.axis_index("z"), core, late]).astype(jnp.int32)

    hidden_pre = jnp.dot(prefix_embed, w_hidden, preferred_element_type=F32) + b_hidden
    tangent = jnp.tanh(hidden_pre)
    hidden = tangent.astype(BF16)
    partial_kv = jnp.einsum("ph,hck->cpk", hidden, w_out, preferred_element_type=F32)
    groups = lax.axis_size("z")
    kv = jnp.concatenate([keys, values], 0)
    partial_kv = partial_kv.reshape(groups, -1, HD).astype(BF16)
    mine = exchange(
        jnp.concatenate([jnp.broadcast_to(kv, (groups, *kv.shape)), partial_kv], 1), "z"
    )
    q = by_head(queries)
    g = by_head(out_grad)
    lent_q = lax.ppermute(queries, "y", [(1, 0)])
    lent_g = lax.ppermute(out_grad, "y", [(1, 0)])
    lent_q = by_head(lent_q)
    lent_g = by_head(lent_g)
    other = shift(mine, "c", 1)
    own = jnp.sum(mine[:, kv.shape[0] :].astype(F32), axis=0)
    own = own + shift(own, "c", 1)
    own = (own + shift(own, "y", 1)).astype(BF16)
    pkv = to_all(own, "z").reshape(2, npre, HD)
    lent_state = lent_sweep(pos, lent_q, lent_g, mine, other)
    lent_state = lax.ppermute(lent_state, "y", [(0, 1)])
    state = sweep(pos, q, g, mine, other)
    grads, stats = prefix_part(pos, q, g, pkv, state, lent_state)
    lent_stats = lax.ppermute(stats, "y", [(1, 0)])
    own_grads = sum_parts(grads, SEQ).astype(BF16)
    prefix_grads = to_all(own_grads, SEQ).reshape(2, npre, HD)
    lent_grad = ()
    for piece in range(PIECES):
        lent_grad = (
            query_grad_piece(True, piece, pos, lent_q, lent_g, lent_stats, mine, other, *lent_grad),
        )
    lent_grad = lax.ppermute(*lent_grad, "y", [(0, 1)])
    query_grad = pkv
    for piece in range(PIECES):
        query_grad = query_grad_piece(False, piece, pos, q, g, stats, mine, other, query_grad)
    query_grad = (query_grad + lent_grad.astype(F32)).astype(BF16)
    grad_w_out = w_out_grad(hidden, prefix_grads)
    hidden_part = jnp.einsum("cpk,hck->ph", prefix_grads, w_out, preferred_element_type=F32)
    parts = to_all(hidden_part.astype(BF16), HEAD)
    hidden_grad = jnp.sum(parts.reshape(heads, npre, units).astype(F32), axis=0)
    pre_grad = hidden_grad * (1.0 - tangent * tangent)
    pre_rounded = pre_grad.astype(BF16)
    embed_part = dot_nt(lax.dynamic_slice_in_dim(pre_rounded, head * share, share, 0), w_hidden)
    own_embed = sum_parts(embed_part, CYZ).astype(BF16)
    near = to_all(own_embed, OWNERS)
    far = shift(near, "c", 1)
    sides = jnp.stack([jnp.where(core == 0, near, far), jnp.where(core == 0, far, near)], 0)
    sides = sides.reshape(2, heads, -1, emb).transpose(1, 0, 2, 3)
    grad_prefix = sides.reshape(npre, emb).astype(F32)
    grad_w_hidden = w_hidden_grad(prefix_embed, pre_rounded)
    grad_b_hidden = jnp.sum(pre_grad, axis=0)
    return (query_grad, grad_w_out, grad_w_hidden, grad_b_hidden, grad_prefix)


def solution(mesh):
    torus = Mesh(mesh.devices.reshape(2, 8, 2, 4, 2), ("y", "z", "c", "x", "w"))
    placed = (
        P(),
        P(None, SEQ),
        P(SEQ),
        P(SEQ, None, HEAD),
        P(SEQ, HEAD),
        P(SEQ, HEAD),
        P(SEQ, HEAD),
        P(SEQ, HEAD),
    )
    return jax.shard_map(
        on_device,
        mesh=torus,
        in_specs=placed,
        out_specs=(P(SEQ, HEAD), P(SEQ, None, HEAD), P(None, SEQ), P(SEQ), P()),
        check_vma=False,
    )
```

```python
import functools
import math

import jax
import jax.numpy as jnp
from jax import lax
from jax.experimental import pallas as pl
from jax.experimental.pallas import tpu as pltpu
from jax.sharding import Mesh
from jax.sharding import PartitionSpec as P

HD = 128
SCALE = 1.0 / math.sqrt(HD)
C1 = SCALE * math.log2(math.e)
NEG = -1e30
TILE = 256
PIECES = 2
SEQ = ("y", "z", "c")
CYZ = ("c", "y", "z")
HEAD = ("x", "w")
OWNERS = ("x", "w", "y", "z")
F32 = jnp.float32
BF16 = jnp.bfloat16
SMEM = pl.BlockSpec(memory_space=pltpu.SMEM)
VMEM = pl.BlockSpec(memory_space=pltpu.VMEM)
GRANT = 16 * 2**20


def dot_nt(a, b):
    return lax.dot_general(a, b, (((1,), (1,)), ((), ())), preferred_element_type=F32)


def dot_nn(a, b):
    return lax.dot_general(a, b, (((1,), (0,)), ((), ())), preferred_element_type=F32)


def dot_tn(a, b):
    return lax.dot_general(a, b, (((0,), (0,)), ((), ())), preferred_element_type=F32)


def span(r):
    return slice(r * TILE, (r + 1) * TILE)


def update(state, s, d):
    m, l, t = state
    s = s.reshape(-1, 8, TILE)
    d = d.reshape(-1, 8, TILE)
    new = jnp.maximum(m, jnp.max(s, axis=0))
    fade = jnp.exp2(m - new)
    w = jnp.exp2(s - new[None])
    return (new, l * fade + jnp.sum(w, axis=0), t * fade + jnp.sum(w * d, axis=0))


def pair_of(kv, j):
    k = jnp.concatenate([kv[2 * j, :HD], kv[2 * j + 1, :HD]], 0)
    v = jnp.concatenate([kv[2 * j, HD : 2 * HD], kv[2 * j + 1, HD : 2 * HD]], 0)
    return k, v


def visible(pos, own, j, shape, key_dim):
    key = lax.broadcasted_iota(jnp.int32, shape, key_dim)
    row = lax.broadcasted_iota(jnp.int32, shape, 1 - key_dim) % HD
    if own:
        return key <= (pos[0] - 2 * j) * HD + row
    return key < (pos[0] + pos[1] - 2 * j) * HD


def sweep_step(pos, q, g, mine, other, j, states, masked=False):
    for own, kv in ((True, mine), (False, other)):
        k, v = pair_of(kv, j)
        seen = visible(pos, own, j, (2 * HD, TILE), 0) if masked else None
        new = []
        for r in range(q.shape[0] // TILE):
            s = dot_nt(k, q[span(r), :]) * C1
            if masked:
                s = jnp.where(seen, s, NEG)
            new.append(update(states[r], s, dot_nt(v, g[span(r), :])))
        states = tuple(new)
    return states


def empty_states(tiles):
    zero = jnp.zeros((8, TILE), F32)
    return tuple((jnp.full((8, TILE), NEG, F32), zero, zero) for _ in range(tiles))


def sweep_kernel(pos, q, g, mine, other, out):
    tiles = q.shape[0] // TILE
    step = functools.partial(sweep_step, pos, q, g, mine, other)
    half = pos[0] // 2
    states = step(half, lax.fori_loop(0, half, step, empty_states(tiles)), True)
    for r in range(tiles):
        for a in range(3):
            out[a, :, span(r)] = states[r][a]


def merged(m, l, t):
    top = jnp.max(m, axis=0, keepdims=True)
    fade = jnp.exp2(m - top)
    return top, jnp.sum(l * fade, axis=0, keepdims=True), jnp.sum(t * fade, axis=0, keepdims=True)


def lent_sweep_kernel(pos, q, g, mine, other, out):
    tiles = q.shape[0] // TILE
    step = functools.partial(sweep_step, pos, q, g, mine, other)
    pairs = jnp.where(pos[2] == 0, mine.shape[0] // 2, 0)
    states = lax.fori_loop(0, pairs, step, empty_states(tiles))
    for r in range(tiles):
        for a, value in enumerate(merged(*states[r])):
            out[a : a + 1, span(r)] = value


def prefix_kernel(pos, q, g, pkv, state, lent, grads, stats):
    npre = pkv.shape[1]
    kg = jnp.zeros((npre, HD), F32)
    vg = jnp.zeros((npre, HD), F32)
    late = pos[2] == 1
    for r in range(q.shape[0] // TILE):
        s = dot_nt(pkv[0], q[span(r), :]) * C1
        d = dot_nt(pkv[1], g[span(r), :])
        near = merged(*update(tuple(state[a, :, span(r)] for a in range(3)), s, d))
        far = tuple(
            jnp.where(late, lent[a : a + 1, span(r)], empty) for a, empty in enumerate((NEG, 0.0, 0.0))
        )
        top = jnp.maximum(near[0], far[0])
        near_fade = jnp.exp2(near[0] - top)
        far_fade = jnp.exp2(far[0] - top)
        total = near[1] * near_fade + far[1] * far_fade
        delta = (near[2] * near_fade + far[2] * far_fade) / total
        log_total = top + jnp.log2(total)
        stats[0:1, span(r)] = log_total
        stats[1:2, span(r)] = delta
        p = jnp.exp2(s - log_total)
        kg = kg + dot_nn((p * (d - delta)).astype(BF16), q[span(r), :])
        vg = vg + dot_nn(p.astype(BF16), g[span(r), :])
    grads[0] = (kg * SCALE).astype(grads.dtype)
    grads[1] = vg.astype(grads.dtype)


def grad_kernel(lent, piece, pos, q, g, stats, mine, other, *refs):
    *extra, out, total, log_total, delta = refs
    rows = q.shape[0]
    pairs = mine.shape[0] // 2 // PIECES
    first = piece * pairs

    def part(k, v, seen=None):
        for r in range(rows // TILE):
            s = dot_nt(q[span(r), :], k) * C1
            if seen is not None:
                s = jnp.where(seen, s, NEG)
            d = dot_nt(g[span(r), :], v)
            pieces = []
            for b in range(k.shape[0] // HD):
                lanes = slice(b * HD, (b + 1) * HD)
                p = jnp.exp2(s[:, lanes] - log_total[span(r), :])
                pieces.append((p * (d[:, lanes] - delta[span(r), :])).astype(BF16))
            total[span(r), :] += dot_nn(jnp.concatenate(pieces, 1), k)

    def step(i, masked=False):
        for own, kv in ((True, mine), (False, other)):
            k, v = pair_of(kv, first + i)
            seen = visible(pos, own, first + i, (TILE, 2 * HD), 1) if masked else None
            part(k, v, seen)

    def spread():
        columns = stats[...].T
        log_total[...] = jnp.broadcast_to(columns[:, 0:1], (rows, HD))
        delta[...] = jnp.broadcast_to(columns[:, 1:2], (rows, HD))

    if lent and piece > 0:
        for h in range(rows // HD):
            at = slice(h * HD, (h + 1) * HD)
            total[at, :] = extra[0][:, at].astype(F32) * (1.0 / SCALE)
    else:
        total[...] = jnp.zeros((rows, HD), F32)
    if lent:

        @pl.when(pos[2] == 0)
        def _():
            spread()
            lax.fori_loop(0, pairs, lambda i, _: step(i), None)

    else:
        spread()
        if piece == 0:
            part(extra[0][0], extra[0][1])
        half = pos[0] // 2
        lax.fori_loop(0, jnp.clip(half - first, 0, pairs), lambda i, _: step(i), None)

        @pl.when((half >= first) & (half < first + pairs))
        def _():
            step(half - first, True)

    for h in range(rows // HD):
        at = slice(h * HD, (h + 1) * HD)
        out[:, at] = (total[at, :] * SCALE).astype(out.dtype)


def call(kernel, out_shape, flops, *values, scratch=()):
    held = [v if v.dtype == jnp.int32 else pltpu.with_memory_space_constraint(v, pltpu.VMEM) for v in values]
    return pl.pallas_call(
        kernel,
        out_shape=out_shape,
        in_specs=[SMEM if v.dtype == jnp.int32 else VMEM for v in values],
        out_specs=jax.tree.map(lambda _: VMEM, out_shape),
        scratch_shapes=list(scratch),
        compiler_params=pltpu.CompilerParams(vmem_limit_bytes=GRANT),
        cost_estimate=pl.CostEstimate(flops=flops, bytes_accessed=10**6, transcendentals=10**6),
    )(*held)


def sweep(pos, q, g, mine, other):
    return call(sweep_kernel, jax.ShapeDtypeStruct((3, 8, q.shape[0]), F32), 10**9, pos, q, g, mine, other)


def lent_sweep(pos, q, g, mine, other):
    out = jax.ShapeDtypeStruct((3, q.shape[0]), F32)
    return call(lent_sweep_kernel, out, 10**9, pos, q, g, mine, other)


def prefix_part(pos, q, g, pkv, state, lent):
    out = (jax.ShapeDtypeStruct(pkv.shape, BF16), jax.ShapeDtypeStruct((2, q.shape[0]), F32))
    return call(prefix_kernel, out, 3 * 10**8, pos, q, g, pkv, state, lent)


def query_grad_piece(lent, piece, pos, q, g, stats, mine, other, *extra):
    out = jax.ShapeDtypeStruct(q.shape[::-1], BF16)
    scratch = [pltpu.VMEM(q.shape, F32)] * 3
    kernel = functools.partial(grad_kernel, lent, piece)
    return call(kernel, out, 10**9, pos, q, g, stats, mine, other, *extra, scratch=scratch)


def w_hidden_kernel(place, embed, *refs):
    *parts, grad_w, grad_b, pre = refs
    lines = len(parts)
    share = parts[0].shape[0] // 2
    for k, part in enumerate(parts):
        line = (place[0] + lines - k) % lines
        for side in range(2):
            source = 2 * line + (place[1] + side) % 2
            pre[pl.ds(pl.multiple_of(source * share, share), share), :] = part[side * share : (side + 1) * share]
    grad_w[...] = dot_tn(embed[...], pre[...])
    grad_b[...] = jnp.sum(pre[...].astype(F32), axis=0)


def w_hidden_grad(place, embed, *parts):
    npre, emb = embed.shape
    units = parts[0].shape[1]
    out = (jax.ShapeDtypeStruct((emb, units), F32), jax.ShapeDtypeStruct((units,), F32))
    scratch = [pltpu.VMEM((npre, units), BF16)]
    return call(w_hidden_kernel, out, 2 * 10**8, place, embed, *parts, scratch=scratch)


def w_out_kernel(hidden, grads, out):
    for c in range(grads.shape[0]):
        out[:, c, :] = dot_tn(hidden[...], grads[c])


def w_out_grad(hidden, grads):
    out = jax.ShapeDtypeStruct((hidden.shape[1], grads.shape[0], HD), F32)
    return call(w_out_kernel, out, 10**8, hidden, grads)


def exchange(value, axes):
    return lax.all_to_all(value, axes, 0, 0, tiled=True)


def to_all(value, axes):
    return exchange(jnp.broadcast_to(value, (lax.axis_size(axes), *value.shape)), axes)


def sum_parts(value, axes, dtype=BF16):
    parts = exchange(value.reshape(lax.axis_size(axes), -1, HD).astype(dtype), axes)
    return jnp.sum(parts.astype(F32), axis=0)


def shift(value, axis, steps):
    count = lax.axis_size(axis)
    return lax.ppermute(value, axis, [(i, (i + steps) % count) for i in range(count)])


def by_head(rows):
    return rows.reshape(rows.shape[0], -1, HD).transpose(1, 0, 2).reshape(-1, HD)


def on_device(prefix_embed, w_hidden, b_hidden, w_out, queries, keys, values, out_grad):
    npre, emb = prefix_embed.shape
    units = w_hidden.shape[1]
    core = lax.axis_index("c")
    late = lax.axis_index("y")
    head = lax.axis_index(HEAD)
    heads = lax.axis_size(HEAD)
    share = npre // heads
    pos = jnp.stack([lax.axis_index("z"), core, late]).astype(jnp.int32)

    hidden_pre = jnp.dot(prefix_embed, w_hidden, preferred_element_type=F32) + b_hidden
    tangent = jnp.tanh(hidden_pre)
    hidden = tangent.astype(BF16)
    partial_kv = jnp.einsum("ph,hck->cpk", hidden, w_out, preferred_element_type=F32)
    groups = lax.axis_size("z")
    kv = jnp.concatenate([keys, values], 0)
    partial_kv = partial_kv.reshape(groups, -1, HD).astype(BF16)
    mine = exchange(
        jnp.concatenate([jnp.broadcast_to(kv, (groups, *kv.shape)), partial_kv], 1), "z"
    )
    q = by_head(queries)
    g = by_head(out_grad)
    lent_q = lax.ppermute(queries, "y", [(1, 0)])
    lent_g = lax.ppermute(out_grad, "y", [(1, 0)])
    lent_q = by_head(lent_q)
    lent_g = by_head(lent_g)
    other = shift(mine, "c", 1)
    own = jnp.sum(mine[:, kv.shape[0] :].astype(F32), axis=0)
    own = own + shift(own, "c", 1)
    own = (own + shift(own, "y", 1)).astype(BF16)
    pkv = to_all(own, "z").reshape(2, npre, HD)
    lent_state = lent_sweep(pos, lent_q, lent_g, mine, other)
    lent_state = lax.ppermute(lent_state, "y", [(0, 1)])
    state = sweep(pos, q, g, mine, other)
    grads, stats = prefix_part(pos, q, g, pkv, state, lent_state)
    lent_stats = lax.ppermute(stats, "y", [(1, 0)])
    prefix_share = sum_parts(grads, SEQ).astype(BF16)
    prefix_grads = to_all(prefix_share, SEQ).reshape(2, npre, HD)
    lent_grad = ()
    for piece in range(PIECES):
        lent_grad = (
            query_grad_piece(True, piece, pos, lent_q, lent_g, lent_stats, mine, other, *lent_grad),
        )
    lent_grad = lax.ppermute(*lent_grad, "y", [(0, 1)])
    own_grads = []
    for piece in range(PIECES):
        first = (pkv,) if piece == 0 else ()
        own_grads.append(query_grad_piece(False, piece, pos, q, g, stats, mine, other, *first))
    query_grad = sum(v.astype(F32) for v in (*own_grads, lent_grad)).astype(BF16)
    grad_w_out = w_out_grad(hidden, prefix_grads)
    hidden_part = jnp.einsum("cpk,hck->ph", prefix_grads, w_out, preferred_element_type=F32)
    parts = exchange(hidden_part.reshape(heads, share, units), HEAD)
    hidden_grad = jnp.sum(parts, axis=0)
    own_tangent = lax.dynamic_slice_in_dim(tangent, head * share, share, 0)
    pre_part = (hidden_grad * (1.0 - own_tangent * own_tangent)).astype(BF16)
    embed_part = dot_nt(pre_part, w_hidden)
    own_embed = sum_parts(embed_part, CYZ).astype(BF16)
    near = to_all(own_embed, OWNERS)
    far = shift(near, "c", 1)
    sides = jnp.stack([jnp.where(core == 0, near, far), jnp.where(core == 0, far, near)], 0)
    sides = sides.reshape(2, heads, -1, emb).transpose(1, 0, 2, 3)
    grad_prefix = sides.reshape(npre, emb).astype(F32)
    both = jnp.concatenate([pre_part, shift(pre_part, "w", 1)], 0)
    turns = [shift(both, "x", k) for k in range(1, lax.axis_size("x"))]
    place = jnp.stack([lax.axis_index("x"), lax.axis_index("w")]).astype(jnp.int32)
    grad_w_hidden, grad_b_hidden = w_hidden_grad(place, prefix_embed, both, *turns)
    return (query_grad, grad_w_out, grad_w_hidden, grad_b_hidden, grad_prefix)


def solution(mesh):
    torus = Mesh(mesh.devices.reshape(2, 8, 2, 4, 2), ("y", "z", "c", "x", "w"))
    placed = (
        P(),
        P(None, SEQ),
        P(SEQ),
        P(SEQ, None, HEAD),
        P(SEQ, HEAD),
        P(SEQ, HEAD),
        P(SEQ, HEAD),
        P(SEQ, HEAD),
    )
    return jax.shard_map(
        on_device,
        mesh=torus,
        in_specs=placed,
        out_specs=(P(SEQ, HEAD), P(SEQ, None, HEAD), P(None, SEQ), P(SEQ), P()),
        check_vma=False,
    )
```

```python
import functools
import math

import jax
import jax.numpy as jnp
from jax import lax
from jax.experimental import pallas as pl
from jax.experimental.pallas import tpu as pltpu
from jax.sharding import Mesh
from jax.sharding import PartitionSpec as P

HD = 128
SCALE = 1.0 / math.sqrt(HD)
C1 = SCALE * math.log2(math.e)
NEG = -1e30
TILE = 256
PIECES = 2
SEQ = ("y", "z", "c")
CYZ = ("c", "y", "z")
HEAD = ("x", "w")
OWNERS = ("x", "w", "y", "z")
F32 = jnp.float32
BF16 = jnp.bfloat16
SMEM = pl.BlockSpec(memory_space=pltpu.SMEM)
VMEM = pl.BlockSpec(memory_space=pltpu.VMEM)
GRANT = 16 * 2**20


def dot_nt(a, b):
    return lax.dot_general(a, b, (((1,), (1,)), ((), ())), preferred_element_type=F32)


def dot_nn(a, b):
    return lax.dot_general(a, b, (((1,), (0,)), ((), ())), preferred_element_type=F32)


def dot_tn(a, b):
    return lax.dot_general(a, b, (((0,), (0,)), ((), ())), preferred_element_type=F32)


def span(r):
    return slice(r * TILE, (r + 1) * TILE)


def update(state, s, d):
    m, l, t = state
    s = s.reshape(-1, 8, TILE)
    d = d.reshape(-1, 8, TILE)
    new = jnp.maximum(m, jnp.max(s, axis=0))
    fade = jnp.exp2(m - new)
    w = jnp.exp2(s - new[None])
    return (new, l * fade + jnp.sum(w, axis=0), t * fade + jnp.sum(w * d, axis=0))


def pair_of(kv, j):
    k = jnp.concatenate([kv[2 * j, :HD], kv[2 * j + 1, :HD]], 0)
    v = jnp.concatenate([kv[2 * j, HD : 2 * HD], kv[2 * j + 1, HD : 2 * HD]], 0)
    return k, v


def visible(pos, own, j, shape, key_dim):
    key = lax.broadcasted_iota(jnp.int32, shape, key_dim)
    row = lax.broadcasted_iota(jnp.int32, shape, 1 - key_dim) % HD
    if own:
        return key <= (pos[0] - 2 * j) * HD + row
    return key < (pos[0] + pos[1] - 2 * j) * HD


def sweep_step(pos, q, g, mine, other, j, states, masked=False):
    for own, kv in ((True, mine), (False, other)):
        k, v = pair_of(kv, j)
        seen = visible(pos, own, j, (2 * HD, TILE), 0) if masked else None
        new = []
        for r in range(q.shape[0] // TILE):
            s = dot_nt(k, q[span(r), :]) * C1
            if masked:
                s = jnp.where(seen, s, NEG)
            new.append(update(states[r], s, dot_nt(v, g[span(r), :])))
        states = tuple(new)
    return states


def empty_states(tiles):
    zero = jnp.zeros((8, TILE), F32)
    return tuple((jnp.full((8, TILE), NEG, F32), zero, zero) for _ in range(tiles))


def sweep_kernel(pos, q, g, mine, other, out):
    tiles = q.shape[0] // TILE
    step = functools.partial(sweep_step, pos, q, g, mine, other)
    half = pos[0] // 2
    states = step(half, lax.fori_loop(0, half, step, empty_states(tiles)), True)
    for r in range(tiles):
        for a in range(3):
            out[a, :, span(r)] = states[r][a]


def merged(m, l, t):
    top = jnp.max(m, axis=0, keepdims=True)
    fade = jnp.exp2(m - top)
    return top, jnp.sum(l * fade, axis=0, keepdims=True), jnp.sum(t * fade, axis=0, keepdims=True)


def lent_sweep_kernel(pos, q, g, mine, other, out):
    tiles = q.shape[0] // TILE
    step = functools.partial(sweep_step, pos, q, g, mine, other)
    pairs = jnp.where(pos[2] == 0, mine.shape[0] // 2, 0)
    states = lax.fori_loop(0, pairs, step, empty_states(tiles))
    for r in range(tiles):
        for a, value in enumerate(merged(*states[r])):
            out[a : a + 1, span(r)] = value


def prefix_kernel(pos, q, g, pkv, state, lent, grads, stats):
    npre = pkv.shape[1]
    kg = jnp.zeros((npre, HD), F32)
    vg = jnp.zeros((npre, HD), F32)
    late = pos[2] == 1
    for r in range(q.shape[0] // TILE):
        s = dot_nt(pkv[0], q[span(r), :]) * C1
        d = dot_nt(pkv[1], g[span(r), :])
        near = merged(*update(tuple(state[a, :, span(r)] for a in range(3)), s, d))
        far = tuple(
            jnp.where(late, lent[a : a + 1, span(r)], empty) for a, empty in enumerate((NEG, 0.0, 0.0))
        )
        top = jnp.maximum(near[0], far[0])
        near_fade = jnp.exp2(near[0] - top)
        far_fade = jnp.exp2(far[0] - top)
        total = near[1] * near_fade + far[1] * far_fade
        delta = (near[2] * near_fade + far[2] * far_fade) / total
        log_total = top + jnp.log2(total)
        stats[0:1, span(r)] = log_total
        stats[1:2, span(r)] = delta
        p = jnp.exp2(s - log_total)
        kg = kg + dot_nn((p * (d - delta)).astype(BF16), q[span(r), :])
        vg = vg + dot_nn(p.astype(BF16), g[span(r), :])
    grads[0] = (kg * SCALE).astype(grads.dtype)
    grads[1] = vg.astype(grads.dtype)


def grad_kernel(lent, piece, pos, q, g, stats, mine, other, *refs):
    *extra, out, total, log_total, delta = refs
    rows = q.shape[0]
    pairs = mine.shape[0] // 2 // PIECES
    first = piece * pairs

    def part(k, v, seen=None):
        for r in range(rows // TILE):
            s = dot_nt(q[span(r), :], k) * C1
            if seen is not None:
                s = jnp.where(seen, s, NEG)
            d = dot_nt(g[span(r), :], v)
            pieces = []
            for b in range(k.shape[0] // HD):
                lanes = slice(b * HD, (b + 1) * HD)
                p = jnp.exp2(s[:, lanes] - log_total[span(r), :])
                pieces.append((p * (d[:, lanes] - delta[span(r), :])).astype(BF16))
            total[span(r), :] += dot_nn(jnp.concatenate(pieces, 1), k)

    def step(i, masked=False):
        for own, kv in ((True, mine), (False, other)):
            k, v = pair_of(kv, first + i)
            seen = visible(pos, own, first + i, (TILE, 2 * HD), 1) if masked else None
            part(k, v, seen)

    def spread():
        columns = stats[...].T
        log_total[...] = jnp.broadcast_to(columns[:, 0:1], (rows, HD))
        delta[...] = jnp.broadcast_to(columns[:, 1:2], (rows, HD))

    if piece > 0:
        for h in range(rows // HD):
            at = slice(h * HD, (h + 1) * HD)
            total[at, :] = extra[0][:, at].astype(F32) * (1.0 / SCALE)
    else:
        total[...] = jnp.zeros((rows, HD), F32)
    if lent:

        @pl.when(pos[2] == 0)
        def _():
            spread()
            lax.fori_loop(0, pairs, lambda i, _: step(i), None)

    else:
        spread()
        if piece == 0:
            part(extra[0][0], extra[0][1])
        half = pos[0] // 2
        lax.fori_loop(0, jnp.clip(half - first, 0, pairs), lambda i, _: step(i), None)

        @pl.when((half >= first) & (half < first + pairs))
        def _():
            step(half - first, True)

    for h in range(rows // HD):
        at = slice(h * HD, (h + 1) * HD)
        out[:, at] = (total[at, :] * SCALE).astype(out.dtype)


def call(kernel, out_shape, flops, *values, scratch=()):
    held = [v if v.dtype == jnp.int32 else pltpu.with_memory_space_constraint(v, pltpu.VMEM) for v in values]
    return pl.pallas_call(
        kernel,
        out_shape=out_shape,
        in_specs=[SMEM if v.dtype == jnp.int32 else VMEM for v in values],
        out_specs=jax.tree.map(lambda _: VMEM, out_shape),
        scratch_shapes=list(scratch),
        compiler_params=pltpu.CompilerParams(vmem_limit_bytes=GRANT),
        cost_estimate=pl.CostEstimate(flops=flops, bytes_accessed=10**6, transcendentals=10**6),
    )(*held)


def sweep(pos, q, g, mine, other):
    return call(sweep_kernel, jax.ShapeDtypeStruct((3, 8, q.shape[0]), F32), 10**9, pos, q, g, mine, other)


def lent_sweep(pos, q, g, mine, other):
    out = jax.ShapeDtypeStruct((3, q.shape[0]), F32)
    return call(lent_sweep_kernel, out, 10**9, pos, q, g, mine, other)


def prefix_part(pos, q, g, pkv, state, lent):
    out = (jax.ShapeDtypeStruct(pkv.shape, BF16), jax.ShapeDtypeStruct((2, q.shape[0]), F32))
    return call(prefix_kernel, out, 3 * 10**8, pos, q, g, pkv, state, lent)


def query_grad_piece(lent, piece, pos, q, g, stats, mine, other, *extra):
    out = jax.ShapeDtypeStruct(q.shape[::-1], BF16)
    scratch = [pltpu.VMEM(q.shape, F32)] * 3
    kernel = functools.partial(grad_kernel, lent, piece)
    return call(kernel, out, 10**9, pos, q, g, stats, mine, other, *extra, scratch=scratch)


def embed_kernel(parts, factor, w_hidden, pre, embed):
    pre[...] = (jnp.sum(parts[...], axis=0) * factor[...]).astype(BF16)
    rows = dot_nt(pre[...], w_hidden[...])
    for k in range(embed.shape[1]):
        embed[:, k, :] = rows[:, k * HD : (k + 1) * HD].astype(BF16)


def embed_rows(parts, factor, w_hidden):
    share = factor.shape[0]
    out = (
        jax.ShapeDtypeStruct(factor.shape, BF16),
        jax.ShapeDtypeStruct((share, w_hidden.shape[0] // HD, HD), BF16),
    )
    return call(embed_kernel, out, 2 * 10**7, parts, factor, w_hidden)


def w_hidden_kernel(place, embed, *refs):
    *parts, grad_w, grad_b, pre = refs
    lines = len(parts)
    share = parts[0].shape[0] // 2
    for k, part in enumerate(parts):
        line = (place[0] + lines - k) % lines
        for side in range(2):
            source = 2 * line + (place[1] + side) % 2
            pre[pl.ds(pl.multiple_of(source * share, share), share), :] = part[side * share : (side + 1) * share]
    grad_w[...] = dot_tn(embed[...], pre[...])
    grad_b[...] = jnp.sum(pre[...].astype(F32), axis=0)


def w_hidden_grad(place, embed, *parts):
    npre, emb = embed.shape
    units = parts[0].shape[1]
    out = (jax.ShapeDtypeStruct((emb, units), F32), jax.ShapeDtypeStruct((units,), F32))
    scratch = [pltpu.VMEM((npre, units), BF16)]
    return call(w_hidden_kernel, out, 2 * 10**8, place, embed, *parts, scratch=scratch)


def w_out_kernel(hidden, grads, out):
    for c in range(grads.shape[0]):
        out[:, c, :] = dot_tn(hidden[...], grads[c])


def w_out_grad(hidden, grads):
    out = jax.ShapeDtypeStruct((hidden.shape[1], grads.shape[0], HD), F32)
    return call(w_out_kernel, out, 10**8, hidden, grads)


def exchange(value, axes):
    return lax.all_to_all(value, axes, 0, 0, tiled=True)


def to_all(value, axes):
    return exchange(jnp.broadcast_to(value, (lax.axis_size(axes), *value.shape)), axes)


def sum_parts(value, axes, dtype=BF16):
    parts = exchange(value.reshape(lax.axis_size(axes), -1, HD).astype(dtype), axes)
    return jnp.sum(parts.astype(F32), axis=0)


def shift(value, axis, steps):
    count = lax.axis_size(axis)
    return lax.ppermute(value, axis, [(i, (i + steps) % count) for i in range(count)])


def by_head(rows):
    return rows.reshape(rows.shape[0], -1, HD).transpose(1, 0, 2).reshape(-1, HD)


def on_device(prefix_embed, w_hidden, b_hidden, w_out, queries, keys, values, out_grad):
    npre, emb = prefix_embed.shape
    units = w_hidden.shape[1]
    core = lax.axis_index("c")
    late = lax.axis_index("y")
    head = lax.axis_index(HEAD)
    heads = lax.axis_size(HEAD)
    share = npre // heads
    pos = jnp.stack([lax.axis_index("z"), core, late]).astype(jnp.int32)

    hidden_pre = jnp.dot(prefix_embed, w_hidden, preferred_element_type=F32) + b_hidden
    tangent = jnp.tanh(hidden_pre)
    hidden = tangent.astype(BF16)
    partial_kv = jnp.einsum("ph,hck->cpk", hidden, w_out, preferred_element_type=F32)
    own_tangent = lax.dynamic_slice_in_dim(tangent, head * share, share, 0)
    factor = lax.optimization_barrier(1.0 - own_tangent * own_tangent)
    groups = lax.axis_size("z")
    kv = jnp.concatenate([keys, values], 0)
    partial_kv = partial_kv.reshape(groups, -1, HD).astype(BF16)
    mine = exchange(
        jnp.concatenate([jnp.broadcast_to(kv, (groups, *kv.shape)), partial_kv], 1), "z"
    )
    q = by_head(queries)
    g = by_head(out_grad)
    lent_q = lax.ppermute(queries, "y", [(1, 0)])
    lent_g = lax.ppermute(out_grad, "y", [(1, 0)])
    lent_q = by_head(lent_q)
    lent_g = by_head(lent_g)
    other = shift(mine, "c", 1)
    sides = [jnp.sum(v[:, kv.shape[0] :].astype(F32), axis=0) for v in (mine, other)]
    own = sides[0] + sides[1]
    own = (own + shift(own, "y", 1)).astype(BF16)
    pkv = to_all(own, "z").reshape(2, npre, HD)
    lent_state = lent_sweep(pos, lent_q, lent_g, mine, other)
    lent_state = lax.ppermute(lent_state, "y", [(0, 1)])
    state = sweep(pos, q, g, mine, other)
    grads, stats = prefix_part(pos, q, g, pkv, state, lent_state)
    lent_stats = lax.ppermute(stats, "y", [(1, 0)])
    prefix_share = sum_parts(grads, SEQ).astype(BF16)
    prefix_grads = to_all(prefix_share, SEQ).reshape(2, npre, HD)
    lent_grad = ()
    for piece in range(PIECES):
        lent_grad = (
            query_grad_piece(True, piece, pos, lent_q, lent_g, lent_stats, mine, other, *lent_grad),
        )
    lent_grad = lax.ppermute(*lent_grad, "y", [(0, 1)])
    own_grad = pkv
    for piece in range(PIECES):
        own_grad = query_grad_piece(False, piece, pos, q, g, stats, mine, other, own_grad)
    query_grad = (own_grad.astype(F32) + lent_grad.astype(F32)).astype(BF16)
    grad_w_out = w_out_grad(hidden, prefix_grads)
    hidden_part = jnp.einsum("cpk,hck->ph", prefix_grads, w_out, preferred_element_type=F32)
    parts = exchange(hidden_part.reshape(heads, share, units), HEAD)
    pre_part, embed_part = embed_rows(parts, factor, w_hidden)
    own_embed = jnp.sum(exchange(embed_part, CYZ).astype(F32), axis=0).astype(BF16)
    near = to_all(own_embed, OWNERS)
    far = shift(near, "c", 1)
    sides = jnp.stack([jnp.where(core == 0, near, far), jnp.where(core == 0, far, near)], 0)
    sides = sides.reshape(2, heads, -1, emb).transpose(1, 0, 2, 3)
    grad_prefix = sides.reshape(npre, emb).astype(F32)
    both = jnp.concatenate([pre_part, shift(pre_part, "w", 1)], 0)
    turns = [shift(both, "x", k) for k in range(1, lax.axis_size("x"))]
    place = jnp.stack([lax.axis_index("x"), lax.axis_index("w")]).astype(jnp.int32)
    grad_w_hidden, grad_b_hidden = w_hidden_grad(place, prefix_embed, both, *turns)
    return (query_grad, grad_w_out, grad_w_hidden, grad_b_hidden, grad_prefix)


def solution(mesh):
    torus = Mesh(mesh.devices.reshape(2, 8, 2, 4, 2), ("y", "z", "c", "x", "w"))
    placed = (
        P(),
        P(None, SEQ),
        P(SEQ),
        P(SEQ, None, HEAD),
        P(SEQ, HEAD),
        P(SEQ, HEAD),
        P(SEQ, HEAD),
        P(SEQ, HEAD),
    )
    return jax.shard_map(
        on_device,
        mesh=torus,
        in_specs=placed,
        out_specs=(P(SEQ, HEAD), P(SEQ, None, HEAD), P(None, SEQ), P(SEQ), P()),
        check_vma=False,
    )
```

```python
import functools
import math

import jax
import jax.numpy as jnp
from jax import lax
from jax.experimental import pallas as pl
from jax.experimental.pallas import tpu as pltpu
from jax.sharding import Mesh
from jax.sharding import PartitionSpec as P

HD = 128
SCALE = 1.0 / math.sqrt(HD)
C1 = SCALE * math.log2(math.e)
NEG = -1e30
TILE = 256
PIECES = 2
TALL = 8
SEQ = ("y", "z", "c")
YZ = ("y", "z")
CYZ = ("c", "y", "z")
HEAD = ("x", "w")
OWNERS = ("x", "w", "y", "z")
F32 = jnp.float32
BF16 = jnp.bfloat16
SMEM = pl.BlockSpec(memory_space=pltpu.SMEM)
VMEM = pl.BlockSpec(memory_space=pltpu.VMEM)
GRANT = 16 * 2**20


def dot_nt(a, b):
    return lax.dot_general(a, b, (((1,), (1,)), ((), ())), preferred_element_type=F32)


def dot_nn(a, b):
    return lax.dot_general(a, b, (((1,), (0,)), ((), ())), preferred_element_type=F32)


def dot_tn(a, b):
    return lax.dot_general(a, b, (((0,), (0,)), ((), ())), preferred_element_type=F32)


def span(r):
    return slice(r * TILE, (r + 1) * TILE)


def update(state, s, d):
    m, l, t = state
    s = s.reshape(-1, 8, TILE)
    d = d.reshape(-1, 8, TILE)
    new = jnp.maximum(m, jnp.max(s, axis=0))
    fade = jnp.exp2(m - new)
    w = jnp.exp2(s - new[None])
    return (new, l * fade + jnp.sum(w, axis=0), t * fade + jnp.sum(w * d, axis=0))


def pair_of(kv, j):
    k = jnp.concatenate([kv[2 * j, :HD], kv[2 * j + 1, :HD]], 0)
    v = jnp.concatenate([kv[2 * j, HD : 2 * HD], kv[2 * j + 1, HD : 2 * HD]], 0)
    return k, v


def visible(pos, own, j, shape, key_dim):
    key = lax.broadcasted_iota(jnp.int32, shape, key_dim)
    row = lax.broadcasted_iota(jnp.int32, shape, 1 - key_dim) % HD
    if own:
        return key <= (pos[0] - 2 * j) * HD + row
    return key < (pos[0] + pos[1] - 2 * j) * HD


def sweep_step(pos, q, g, mine, other, j, states, masked=False):
    for own, kv in ((True, mine), (False, other)):
        k, v = pair_of(kv, j)
        seen = visible(pos, own, j, (2 * HD, TILE), 0) if masked else None
        new = []
        for r in range(q.shape[0] // TILE):
            s = dot_nt(k, q[span(r), :]) * C1
            if masked:
                s = jnp.where(seen, s, NEG)
            new.append(update(states[r], s, dot_nt(v, g[span(r), :])))
        states = tuple(new)
    return states


def empty_states(tiles):
    zero = jnp.zeros((8, TILE), F32)
    return tuple((jnp.full((8, TILE), NEG, F32), zero, zero) for _ in range(tiles))


def sweep_kernel(pos, q, g, mine, other, out):
    tiles = q.shape[0] // TILE
    step = functools.partial(sweep_step, pos, q, g, mine, other)
    half = pos[0] // 2
    states = step(half, lax.fori_loop(0, half, step, empty_states(tiles)), True)
    for r in range(tiles):
        for a in range(3):
            out[a, :, span(r)] = states[r][a]


def merged(m, l, t):
    top = jnp.max(m, axis=0, keepdims=True)
    fade = jnp.exp2(m - top)
    return top, jnp.sum(l * fade, axis=0, keepdims=True), jnp.sum(t * fade, axis=0, keepdims=True)


def lent_sweep_kernel(pos, q, g, mine, other, out):
    tiles = q.shape[0] // TILE
    step = functools.partial(sweep_step, pos, q, g, mine, other)
    pairs = jnp.where(pos[2] == 0, mine.shape[0] // 2, 0)
    states = lax.fori_loop(0, pairs, step, empty_states(tiles))
    for r in range(tiles):
        for a, value in enumerate(merged(*states[r])):
            out[a : a + 1, span(r)] = value


def prefix_kernel(pos, q, g, halves, state, lent, grads, stats, pkv):
    npre = pkv.shape[1]
    pkv[...] = (halves[0].astype(F32) + halves[1].astype(F32)).astype(BF16)
    kg = jnp.zeros((npre, HD), F32)
    vg = jnp.zeros((npre, HD), F32)
    late = pos[2] == 1
    for r in range(q.shape[0] // TILE):
        s = dot_nt(pkv[0], q[span(r), :]) * C1
        d = dot_nt(pkv[1], g[span(r), :])
        near = merged(*update(tuple(state[a, :, span(r)] for a in range(3)), s, d))
        far = tuple(
            jnp.where(late, lent[a : a + 1, span(r)], empty) for a, empty in enumerate((NEG, 0.0, 0.0))
        )
        top = jnp.maximum(near[0], far[0])
        near_fade = jnp.exp2(near[0] - top)
        far_fade = jnp.exp2(far[0] - top)
        total = near[1] * near_fade + far[1] * far_fade
        delta = (near[2] * near_fade + far[2] * far_fade) / total
        log_total = top + jnp.log2(total)
        stats[0:1, span(r)] = log_total
        stats[1:2, span(r)] = delta
        p = jnp.exp2(s - log_total)
        kg = kg + dot_nn((p * (d - delta)).astype(BF16), q[span(r), :])
        vg = vg + dot_nn(p.astype(BF16), g[span(r), :])
    grads[0] = (kg * SCALE).astype(grads.dtype)
    grads[1] = vg.astype(grads.dtype)


def grad_kernel(lent, piece, pos, q, g, stats, mine, other, *refs):
    *extra, out, total, log_total, delta = refs
    rows = q.shape[0]
    pairs = mine.shape[0] // 2 // PIECES
    first = piece * pairs

    def part(k, v, seen=None):
        for r in range(rows // TILE):
            s = dot_nt(q[span(r), :], k) * C1
            if seen is not None:
                s = jnp.where(seen, s, NEG)
            d = dot_nt(g[span(r), :], v)
            pieces = []
            for b in range(k.shape[0] // HD):
                lanes = slice(b * HD, (b + 1) * HD)
                p = jnp.exp2(s[:, lanes] - log_total[span(r), :])
                pieces.append((p * (d[:, lanes] - delta[span(r), :])).astype(BF16))
            total[span(r), :] += dot_nn(jnp.concatenate(pieces, 1), k)

    def step(i, masked=False):
        for own, kv in ((True, mine), (False, other)):
            k, v = pair_of(kv, first + i)
            seen = visible(pos, own, first + i, (TILE, 2 * HD), 1) if masked else None
            part(k, v, seen)

    def spread():
        columns = stats[...].T
        log_total[...] = jnp.broadcast_to(columns[:, 0:1], (rows, HD))
        delta[...] = jnp.broadcast_to(columns[:, 1:2], (rows, HD))

    if piece > 0:
        for h in range(rows // HD):
            at = slice(h * HD, (h + 1) * HD)
            total[at, :] = extra[0][:, at].astype(F32) * (1.0 / SCALE)
    else:
        total[...] = jnp.zeros((rows, HD), F32)
    if lent:

        @pl.when(pos[2] == 0)
        def _():
            spread()
            lax.fori_loop(0, pairs, lambda i, _: step(i), None)

    else:
        spread()
        if piece == 0:
            part(extra[0][0], extra[0][1])
        half = pos[0] // 2
        lax.fori_loop(0, jnp.clip(half - first, 0, pairs), lambda i, _: step(i), None)

        @pl.when((half >= first) & (half < first + pairs))
        def _():
            step(half - first, True)

    for h in range(rows // HD):
        at = slice(h * HD, (h + 1) * HD)
        out[:, at] = (total[at, :] * SCALE).astype(out.dtype)


def call(kernel, out_shape, flops, *values, scratch=()):
    held = [v if v.dtype == jnp.int32 else pltpu.with_memory_space_constraint(v, pltpu.VMEM) for v in values]
    return pl.pallas_call(
        kernel,
        out_shape=out_shape,
        in_specs=[SMEM if v.dtype == jnp.int32 else VMEM for v in values],
        out_specs=jax.tree.map(lambda _: VMEM, out_shape),
        scratch_shapes=list(scratch),
        compiler_params=pltpu.CompilerParams(vmem_limit_bytes=GRANT),
        cost_estimate=pl.CostEstimate(flops=flops, bytes_accessed=10**6, transcendentals=10**6),
    )(*held)


def sweep(pos, q, g, mine, other):
    return call(sweep_kernel, jax.ShapeDtypeStruct((3, 8, q.shape[0]), F32), 10**9, pos, q, g, mine, other)


def lent_sweep(pos, q, g, mine, other):
    out = jax.ShapeDtypeStruct((3, q.shape[0]), F32)
    return call(lent_sweep_kernel, out, 10**9, pos, q, g, mine, other)


def prefix_part(pos, q, g, halves, state, lent):
    pair = jax.ShapeDtypeStruct(halves.shape[1:], BF16)
    out = (pair, jax.ShapeDtypeStruct((2, q.shape[0]), F32), pair)
    return call(prefix_kernel, out, 3 * 10**8, pos, q, g, halves, state, lent)


def query_grad_piece(lent, piece, pos, q, g, stats, mine, other, *extra):
    out = jax.ShapeDtypeStruct(q.shape[::-1], BF16)
    scratch = [pltpu.VMEM(q.shape, F32)] * 3
    kernel = functools.partial(grad_kernel, lent, piece)
    return call(kernel, out, 10**9, pos, q, g, stats, mine, other, *extra, scratch=scratch)


def embed_kernel(parts, factor, w_hidden, pre, embed):
    pre[...] = (jnp.sum(parts[...], axis=0) * factor[...]).astype(BF16)
    rows = dot_nt(pre[...], w_hidden[...])
    tall = embed.shape[1]
    wide = rows.shape[1] // HD
    for t in range(embed.shape[0]):
        down, right = t // wide * tall, t % wide * HD
        embed[t] = rows[down : down + tall, right : right + HD].astype(BF16)


def embed_rows(parts, factor, w_hidden):
    share = factor.shape[0]
    out = (
        jax.ShapeDtypeStruct(factor.shape, BF16),
        jax.ShapeDtypeStruct((share * w_hidden.shape[0] // HD // TALL, TALL, HD), BF16),
    )
    return call(embed_kernel, out, 2 * 10**7, parts, factor, w_hidden)


def joined_kernel(heads, pos, near, far, out):
    wide = out.shape[1] // HD
    per_head = near.shape[0] // heads
    first = pos[1] == 0
    for t in range(near.shape[0]):
        pair = (near[t].astype(F32), far[t].astype(F32))
        for side in range(2):
            tile = t // per_head * 2 * per_head + side * per_head + t % per_head
            down, right = tile // wide * TALL, tile % wide * HD
            value = jnp.where(first, pair[side], pair[1 - side])
            out[down : down + TALL, right : right + HD] = value


def joined(pos, near, far, heads, npre, emb):
    out = jax.ShapeDtypeStruct((npre, emb), F32)
    return call(functools.partial(joined_kernel, heads), out, 10**6, pos, near, far)


def w_hidden_kernel(place, embed, *refs):
    *parts, grad_w, grad_b, pre = refs
    lines = len(parts)
    share = parts[0].shape[0] // 2
    for k, part in enumerate(parts):
        line = (place[0] + lines - k) % lines
        for side in range(2):
            source = 2 * line + (place[1] + side) % 2
            pre[pl.ds(pl.multiple_of(source * share, share), share), :] = part[side * share : (side + 1) * share]
    grad_w[...] = dot_tn(embed[...], pre[...])
    grad_b[...] = jnp.sum(pre[...].astype(F32), axis=0)


def w_hidden_grad(place, embed, *parts):
    npre, emb = embed.shape
    units = parts[0].shape[1]
    out = (jax.ShapeDtypeStruct((emb, units), F32), jax.ShapeDtypeStruct((units,), F32))
    scratch = [pltpu.VMEM((npre, units), BF16)]
    return call(w_hidden_kernel, out, 2 * 10**8, place, embed, *parts, scratch=scratch)


def w_out_kernel(hidden, grads, out):
    for c in range(grads.shape[0]):
        out[:, c, :] = dot_tn(hidden[...], grads[c])


def w_out_grad(hidden, grads):
    out = jax.ShapeDtypeStruct((hidden.shape[1], grads.shape[0], HD), F32)
    return call(w_out_kernel, out, 10**8, hidden, grads)


def exchange(value, axes):
    return lax.all_to_all(value, axes, 0, 0, tiled=True)


def to_all(value, axes):
    return exchange(jnp.broadcast_to(value, (lax.axis_size(axes), *value.shape)), axes)


def sum_parts(value, axes, dtype=BF16):
    parts = exchange(value.reshape(lax.axis_size(axes), -1, HD).astype(dtype), axes)
    return jnp.sum(parts.astype(F32), axis=0)


def shift(value, axis, steps):
    count = lax.axis_size(axis)
    return lax.ppermute(value, axis, [(i, (i + steps) % count) for i in range(count)])


def by_head(rows):
    return rows.reshape(rows.shape[0], -1, HD).transpose(1, 0, 2).reshape(-1, HD)


def on_device(prefix_embed, w_hidden, b_hidden, w_out, queries, keys, values, out_grad):
    npre, emb = prefix_embed.shape
    units = w_hidden.shape[1]
    core = lax.axis_index("c")
    late = lax.axis_index("y")
    head = lax.axis_index(HEAD)
    heads = lax.axis_size(HEAD)
    share = npre // heads
    pos = jnp.stack([lax.axis_index("z"), core, late]).astype(jnp.int32)

    hidden_pre = jnp.dot(prefix_embed, w_hidden, preferred_element_type=F32) + b_hidden
    tangent = jnp.tanh(hidden_pre)
    hidden = tangent.astype(BF16)
    partial_kv = jnp.einsum("ph,hck->cpk", hidden, w_out, preferred_element_type=F32)
    own_tangent = lax.dynamic_slice_in_dim(tangent, head * share, share, 0)
    factor = lax.optimization_barrier(1.0 - own_tangent * own_tangent)
    groups = lax.axis_size("z")
    kv = jnp.concatenate([keys, values], 0)
    partial_kv = partial_kv.reshape(groups, -1, HD).astype(BF16)
    mine = exchange(
        jnp.concatenate([jnp.broadcast_to(kv, (groups, *kv.shape)), partial_kv], 1), "z"
    )
    q = by_head(queries)
    g = by_head(out_grad)
    lent_q = lax.ppermute(queries, "y", [(1, 0)])
    lent_g = lax.ppermute(out_grad, "y", [(1, 0)])
    lent_q = by_head(lent_q)
    lent_g = by_head(lent_g)
    other = shift(mine, "c", 1)
    sides = [jnp.sum(v[:, kv.shape[0] :].astype(F32), axis=0) for v in (mine, other)]
    own = (sides[0] + sides[1]).astype(BF16)
    halves = to_all(own, YZ).reshape(lax.axis_size("y"), 2, npre, HD)
    lent_state = lent_sweep(pos, lent_q, lent_g, mine, other)
    lent_state = lax.ppermute(lent_state, "y", [(0, 1)])
    state = sweep(pos, q, g, mine, other)
    grads, stats, pkv = prefix_part(pos, q, g, halves, state, lent_state)
    lent_stats = lax.ppermute(stats, "y", [(1, 0)])
    prefix_share = sum_parts(grads, SEQ).astype(BF16)
    prefix_grads = to_all(prefix_share, SEQ).reshape(2, npre, HD)
    lent_grad = ()
    for piece in range(PIECES):
        lent_grad = (
            query_grad_piece(True, piece, pos, lent_q, lent_g, lent_stats, mine, other, *lent_grad),
        )
    lent_grad = lax.ppermute(*lent_grad, "y", [(0, 1)])
    own_grad = pkv
    for piece in range(PIECES):
        own_grad = query_grad_piece(False, piece, pos, q, g, stats, mine, other, own_grad)
    query_grad = (own_grad.astype(F32) + lent_grad.astype(F32)).astype(BF16)
    grad_w_out = w_out_grad(hidden, prefix_grads)
    hidden_part = jnp.einsum("cpk,hck->ph", prefix_grads, w_out, preferred_element_type=F32)
    parts = exchange(hidden_part.reshape(heads, share, units), HEAD)
    pre_part, embed_part = embed_rows(parts, factor, w_hidden)
    own_embed = jnp.sum(exchange(embed_part, CYZ).astype(F32), axis=0).astype(BF16)
    near = to_all(own_embed, OWNERS)
    far = shift(near, "c", 1)
    grad_prefix = joined(pos, near, far, heads, npre, emb)
    both = jnp.concatenate([pre_part, shift(pre_part, "w", 1)], 0)
    turns = [shift(both, "x", k) for k in range(1, lax.axis_size("x"))]
    place = jnp.stack([lax.axis_index("x"), lax.axis_index("w")]).astype(jnp.int32)
    grad_w_hidden, grad_b_hidden = w_hidden_grad(place, prefix_embed, both, *turns)
    return (query_grad, grad_w_out, grad_w_hidden, grad_b_hidden, grad_prefix)


def solution(mesh):
    torus = Mesh(mesh.devices.reshape(2, 8, 2, 4, 2), ("y", "z", "c", "x", "w"))
    placed = (
        P(),
        P(None, SEQ),
        P(SEQ),
        P(SEQ, None, HEAD),
        P(SEQ, HEAD),
        P(SEQ, HEAD),
        P(SEQ, HEAD),
        P(SEQ, HEAD),
    )
    return jax.shard_map(
        on_device,
        mesh=torus,
        in_specs=placed,
        out_specs=(P(SEQ, HEAD), P(SEQ, None, HEAD), P(None, SEQ), P(SEQ), P()),
        check_vma=False,
    )
```

```python
import functools
import math

import jax
import jax.numpy as jnp
from jax import lax
from jax.experimental import pallas as pl
from jax.experimental.pallas import tpu as pltpu
from jax.sharding import Mesh
from jax.sharding import PartitionSpec as P

HD = 128
SCALE = 1.0 / math.sqrt(HD)
C1 = SCALE * math.log2(math.e)
NEG = -1e30
TILE = 256
PIECES = 2
TALL = 8
SEQ = ("y", "z", "c")
YZ = ("y", "z")
CYZ = ("c", "y", "z")
HEAD = ("x", "w")
OWNERS = ("x", "w", "y", "z")
F32 = jnp.float32
BF16 = jnp.bfloat16
SMEM = pl.BlockSpec(memory_space=pltpu.SMEM)
VMEM = pl.BlockSpec(memory_space=pltpu.VMEM)
GRANT = 16 * 2**20


def dot_nt(a, b):
    return lax.dot_general(a, b, (((1,), (1,)), ((), ())), preferred_element_type=F32)


def dot_nn(a, b):
    return lax.dot_general(a, b, (((1,), (0,)), ((), ())), preferred_element_type=F32)


def dot_tn(a, b):
    return lax.dot_general(a, b, (((0,), (0,)), ((), ())), preferred_element_type=F32)


def span(r):
    return slice(r * TILE, (r + 1) * TILE)


def update(state, s, d):
    m, l, t = state
    s = s.reshape(-1, 8, TILE)
    d = d.reshape(-1, 8, TILE)
    new = jnp.maximum(m, jnp.max(s, axis=0))
    fade = jnp.exp2(m - new)
    w = jnp.exp2(s - new[None])
    return (new, l * fade + jnp.sum(w, axis=0), t * fade + jnp.sum(w * d, axis=0))


def pair_of(kv, j):
    k = jnp.concatenate([kv[2 * j, :HD], kv[2 * j + 1, :HD]], 0)
    v = jnp.concatenate([kv[2 * j, HD : 2 * HD], kv[2 * j + 1, HD : 2 * HD]], 0)
    return k, v


def visible(pos, own, j, shape, key_dim):
    key = lax.broadcasted_iota(jnp.int32, shape, key_dim)
    row = lax.broadcasted_iota(jnp.int32, shape, 1 - key_dim) % HD
    if own:
        return key <= (pos[0] - 2 * j) * HD + row
    return key < (pos[0] + pos[1] - 2 * j) * HD


def generate_kernel(place, embed, w_hidden, bias, w_out, keys, values, hidden, factor, payload, tangent):
    tangent[...] = jnp.tanh(dot_nn(embed[...], w_hidden[...]) + bias[...])
    hidden[...] = tangent[...].astype(BF16)
    share = factor.shape[0]
    first = pl.multiple_of((2 * place[0] + place[1]) * share, share)
    own = tangent[pl.ds(first, share), :]
    factor[...] = 1.0 - own * own
    groups = payload.shape[0]
    rows = keys.shape[0]
    npre = hidden.shape[0]
    size = 2 * npre // groups
    for c in range(2):
        part = dot_nn(hidden[...], w_out[:, c, :]).astype(BF16)
        for k in range(groups // 2):
            payload[c * groups // 2 + k, 2 * rows :, :] = part[k * size : (k + 1) * size]
    for k in range(groups):
        payload[k, :rows, :] = keys[...]
        payload[k, rows : 2 * rows, :] = values[...]


def generated(place, embed, w_hidden, bias, w_out, keys, values):
    npre, units = embed.shape[0], w_hidden.shape[1]
    groups = lax.axis_size("z")
    out = (
        jax.ShapeDtypeStruct((npre, units), BF16),
        jax.ShapeDtypeStruct((npre // lax.axis_size(HEAD), units), F32),
        jax.ShapeDtypeStruct((groups, 2 * keys.shape[0] + 2 * npre // groups, HD), BF16),
    )
    values_in = (embed, w_hidden, bias, w_out, keys, values)
    return pl.pallas_call(
        generate_kernel,
        out_shape=out,
        in_specs=[SMEM] + [whole(v) for v in values_in],
        out_specs=tuple(whole(v) for v in out),
        grid=(1,),
        scratch_shapes=[pltpu.VMEM((npre, units), F32)],
        compiler_params=pltpu.CompilerParams(vmem_limit_bytes=GRANT),
        cost_estimate=pl.CostEstimate(flops=2 * 10**8, bytes_accessed=2 * 10**6, transcendentals=10**5),
        name="generate",
    )(place, *(pltpu.with_memory_space_constraint(v, pltpu.HBM) for v in values_in))


def whole(value):
    return pl.BlockSpec(value.shape, lambda *_: (0,) * len(value.shape))


def sweep_step(pos, q, g, sources, j, states, masked=False):
    for own, kv in sources:
        k, v = pair_of(kv, j)
        seen = visible(pos, own, j, (2 * HD, TILE), 0) if masked else None
        new = []
        for r in range(q.shape[0] // TILE):
            s = dot_nt(k, q[span(r), :]) * C1
            if masked:
                s = jnp.where(seen, s, NEG)
            new.append(update(states[r], s, dot_nt(v, g[span(r), :])))
        states = tuple(new)
    return states


def empty_states(tiles):
    zero = jnp.zeros((8, TILE), F32)
    return tuple((jnp.full((8, TILE), NEG, F32), zero, zero) for _ in range(tiles))


def sweep_kernel(pos, q, g, mine, other, out):
    tiles = q.shape[0] // TILE
    step = functools.partial(sweep_step, pos, q, g, ((True, mine), (False, other)))
    half = pos[0] // 2
    states = step(half, lax.fori_loop(0, half, step, empty_states(tiles)), True)
    for r in range(tiles):
        for a in range(3):
            out[a, :, span(r)] = states[r][a]


def merged(m, l, t):
    top = jnp.max(m, axis=0, keepdims=True)
    fade = jnp.exp2(m - top)
    return top, jnp.sum(l * fade, axis=0, keepdims=True), jnp.sum(t * fade, axis=0, keepdims=True)


def lent_sweep_kernel(last, pos, q, g, kv, *refs):
    *begun, out = refs
    tiles = q.shape[0] // TILE
    states = empty_states(tiles)
    if begun:
        states = tuple(tuple(begun[0][a, :, span(r)] for a in range(3)) for r in range(tiles))
    step = functools.partial(sweep_step, pos, q, g, ((True, kv),))
    pairs = jnp.where(pos[2] == 0, kv.shape[0] // 2, 0)
    states = lax.fori_loop(0, pairs, step, states)
    for r in range(tiles):
        if last:
            for a, value in enumerate(merged(*states[r])):
                out[a : a + 1, span(r)] = value
        else:
            for a in range(3):
                out[a, :, span(r)] = states[r][a]


def prefix_kernel(pos, q, g, halves, state, lent, grads, stats, pkv):
    npre = pkv.shape[1]
    pkv[...] = (halves[0].astype(F32) + halves[1].astype(F32)).astype(BF16)
    kg = jnp.zeros((npre, HD), F32)
    vg = jnp.zeros((npre, HD), F32)
    late = pos[2] == 1
    for r in range(q.shape[0] // TILE):
        s = dot_nt(pkv[0], q[span(r), :]) * C1
        d = dot_nt(pkv[1], g[span(r), :])
        near = merged(*update(tuple(state[a, :, span(r)] for a in range(3)), s, d))
        far = tuple(
            jnp.where(late, lent[a : a + 1, span(r)], empty) for a, empty in enumerate((NEG, 0.0, 0.0))
        )
        top = jnp.maximum(near[0], far[0])
        near_fade = jnp.exp2(near[0] - top)
        far_fade = jnp.exp2(far[0] - top)
        total = near[1] * near_fade + far[1] * far_fade
        delta = (near[2] * near_fade + far[2] * far_fade) / total
        log_total = top + jnp.log2(total)
        stats[0:1, span(r)] = log_total
        stats[1:2, span(r)] = delta
        p = jnp.exp2(s - log_total)
        kg = kg + dot_nn((p * (d - delta)).astype(BF16), q[span(r), :])
        vg = vg + dot_nn(p.astype(BF16), g[span(r), :])
    grads[0] = (kg * SCALE).astype(grads.dtype)
    grads[1] = vg.astype(grads.dtype)


def grad_kernel(lent, piece, pos, q, g, stats, mine, other, *refs):
    *extra, out, total, log_total, delta = refs
    rows = q.shape[0]
    pairs = mine.shape[0] // 2 // PIECES
    first = piece * pairs

    def part(k, v, seen=None):
        for r in range(rows // TILE):
            s = dot_nt(q[span(r), :], k) * C1
            if seen is not None:
                s = jnp.where(seen, s, NEG)
            d = dot_nt(g[span(r), :], v)
            pieces = []
            for b in range(k.shape[0] // HD):
                lanes = slice(b * HD, (b + 1) * HD)
                p = jnp.exp2(s[:, lanes] - log_total[span(r), :])
                pieces.append((p * (d[:, lanes] - delta[span(r), :])).astype(BF16))
            total[span(r), :] += dot_nn(jnp.concatenate(pieces, 1), k)

    def step(i, masked=False):
        for own, kv in ((True, mine), (False, other)):
            k, v = pair_of(kv, first + i)
            seen = visible(pos, own, first + i, (TILE, 2 * HD), 1) if masked else None
            part(k, v, seen)

    def spread():
        columns = stats[...].T
        log_total[...] = jnp.broadcast_to(columns[:, 0:1], (rows, HD))
        delta[...] = jnp.broadcast_to(columns[:, 1:2], (rows, HD))

    if piece > 0:
        for h in range(rows // HD):
            at = slice(h * HD, (h + 1) * HD)
            total[at, :] = extra[0][:, at].astype(F32) * (1.0 / SCALE)
    else:
        total[...] = jnp.zeros((rows, HD), F32)
    if lent:

        @pl.when(pos[2] == 0)
        def _():
            spread()
            lax.fori_loop(0, pairs, lambda i, _: step(i), None)

    else:
        spread()
        if piece == 0:
            part(extra[0][0], extra[0][1])
        half = pos[0] // 2
        lax.fori_loop(0, jnp.clip(half - first, 0, pairs), lambda i, _: step(i), None)

        @pl.when((half >= first) & (half < first + pairs))
        def _():
            step(half - first, True)

    for h in range(rows // HD):
        at = slice(h * HD, (h + 1) * HD)
        out[:, at] = (total[at, :] * SCALE).astype(out.dtype)


def call(kernel, out_shape, flops, *values, scratch=()):
    held = [v if v.dtype == jnp.int32 else pltpu.with_memory_space_constraint(v, pltpu.VMEM) for v in values]
    return pl.pallas_call(
        kernel,
        out_shape=out_shape,
        in_specs=[SMEM if v.dtype == jnp.int32 else VMEM for v in values],
        out_specs=jax.tree.map(lambda _: VMEM, out_shape),
        scratch_shapes=list(scratch),
        compiler_params=pltpu.CompilerParams(vmem_limit_bytes=GRANT),
        cost_estimate=pl.CostEstimate(flops=flops, bytes_accessed=10**6, transcendentals=10**6),
    )(*held)


def sweep(pos, q, g, mine, other):
    return call(sweep_kernel, jax.ShapeDtypeStruct((3, 8, q.shape[0]), F32), 10**9, pos, q, g, mine, other)


def lent_sweep(pos, q, g, kv, *begun):
    last = bool(begun)
    out = jax.ShapeDtypeStruct((3, q.shape[0]) if last else (3, 8, q.shape[0]), F32)
    kernel = functools.partial(lent_sweep_kernel, last)
    return call(kernel, out, 5 * 10**8, pos, q, g, kv, *begun)


def prefix_part(pos, q, g, halves, state, lent):
    pair = jax.ShapeDtypeStruct(halves.shape[1:], BF16)
    out = (pair, jax.ShapeDtypeStruct((2, q.shape[0]), F32), pair)
    return call(prefix_kernel, out, 3 * 10**8, pos, q, g, halves, state, lent)


def query_grad_piece(lent, piece, pos, q, g, stats, mine, other, *extra):
    out = jax.ShapeDtypeStruct(q.shape[::-1], BF16)
    scratch = [pltpu.VMEM(q.shape, F32)] * 3
    kernel = functools.partial(grad_kernel, lent, piece)
    return call(kernel, out, 10**9, pos, q, g, stats, mine, other, *extra, scratch=scratch)


def embed_kernel(parts, factor, w_hidden, pre, embed):
    pre[...] = (jnp.sum(parts[...], axis=0) * factor[...]).astype(BF16)
    rows = dot_nt(pre[...], w_hidden[...])
    tall = embed.shape[1]
    wide = rows.shape[1] // HD
    for t in range(embed.shape[0]):
        down, right = t // wide * tall, t % wide * HD
        embed[t] = rows[down : down + tall, right : right + HD].astype(BF16)


def embed_rows(parts, factor, w_hidden):
    share = factor.shape[0]
    out = (
        jax.ShapeDtypeStruct(factor.shape, BF16),
        jax.ShapeDtypeStruct((share * w_hidden.shape[0] // HD // TALL, TALL, HD), BF16),
    )
    return call(embed_kernel, out, 2 * 10**7, parts, factor, w_hidden)


def joined_kernel(heads, pos, near, far, out):
    wide = out.shape[1] // HD
    per_head = near.shape[0] // heads
    first = pos[1] == 0
    for t in range(near.shape[0]):
        pair = (near[t].astype(F32), far[t].astype(F32))
        for side in range(2):
            tile = t // per_head * 2 * per_head + side * per_head + t % per_head
            down, right = tile // wide * TALL, tile % wide * HD
            value = jnp.where(first, pair[side], pair[1 - side])
            out[down : down + TALL, right : right + HD] = value


def joined(pos, near, far, heads, npre, emb):
    out = jax.ShapeDtypeStruct((npre, emb), F32)
    return call(functools.partial(joined_kernel, heads), out, 10**6, pos, near, far)


def w_hidden_kernel(place, embed, *refs):
    *parts, grad_w, grad_b, pre = refs
    lines = len(parts)
    share = parts[0].shape[0] // 2
    for k, part in enumerate(parts):
        line = (place[0] + lines - k) % lines
        for side in range(2):
            source = 2 * line + (place[1] + side) % 2
            pre[pl.ds(pl.multiple_of(source * share, share), share), :] = part[side * share : (side + 1) * share]
    grad_w[...] = dot_tn(embed[...], pre[...])
    grad_b[...] = jnp.sum(pre[...].astype(F32), axis=0)


def w_hidden_grad(place, embed, *parts):
    npre, emb = embed.shape
    units = parts[0].shape[1]
    out = (jax.ShapeDtypeStruct((emb, units), F32), jax.ShapeDtypeStruct((units,), F32))
    scratch = [pltpu.VMEM((npre, units), BF16)]
    return call(w_hidden_kernel, out, 2 * 10**8, place, embed, *parts, scratch=scratch)


def w_out_kernel(hidden, grads, out):
    for c in range(grads.shape[0]):
        out[:, c, :] = dot_tn(hidden[...], grads[c])


def w_out_grad(hidden, grads):
    out = jax.ShapeDtypeStruct((hidden.shape[1], grads.shape[0], HD), F32)
    return call(w_out_kernel, out, 10**8, hidden, grads)


def exchange(value, axes):
    return lax.all_to_all(value, axes, 0, 0, tiled=True)


def to_all(value, axes):
    return exchange(jnp.broadcast_to(value, (lax.axis_size(axes), *value.shape)), axes)


def sum_parts(value, axes, dtype=BF16):
    parts = exchange(value.reshape(lax.axis_size(axes), -1, HD).astype(dtype), axes)
    return jnp.sum(parts.astype(F32), axis=0)


def shift(value, axis, steps):
    count = lax.axis_size(axis)
    return lax.ppermute(value, axis, [(i, (i + steps) % count) for i in range(count)])


def by_head(rows):
    return rows.reshape(rows.shape[0], -1, HD).transpose(1, 0, 2).reshape(-1, HD)


def on_device(prefix_embed, w_hidden, b_hidden, w_out, queries, keys, values, out_grad):
    npre, emb = prefix_embed.shape
    units = w_hidden.shape[1]
    core = lax.axis_index("c")
    late = lax.axis_index("y")
    heads = lax.axis_size(HEAD)
    share = npre // heads
    place = jnp.stack([lax.axis_index("x"), lax.axis_index("w")]).astype(jnp.int32)
    pos = jnp.stack([lax.axis_index("z"), core, late]).astype(jnp.int32)

    hidden, factor, payload = generated(place, prefix_embed, w_hidden, b_hidden.reshape(1, units), w_out, keys, values)
    kv_rows = 2 * keys.shape[0]
    mine = exchange(payload, "z")
    q = by_head(queries)
    g = by_head(out_grad)
    lent_q = lax.ppermute(queries, "y", [(1, 0)])
    lent_g = lax.ppermute(out_grad, "y", [(1, 0)])
    lent_q = by_head(lent_q)
    lent_g = by_head(lent_g)
    other = shift(mine, "c", 1)
    lent_state = lent_sweep(pos, lent_q, lent_g, mine)
    sides = [jnp.sum(v[:, kv_rows:].astype(F32), axis=0) for v in (mine, other)]
    own = (sides[0] + sides[1]).astype(BF16)
    halves = to_all(own, YZ).reshape(lax.axis_size("y"), 2, npre, HD)
    lent_state = lent_sweep(pos, lent_q, lent_g, other, lent_state)
    lent_state = lax.ppermute(lent_state, "y", [(0, 1)])
    state = sweep(pos, q, g, mine, other)
    grads, stats, pkv = prefix_part(pos, q, g, halves, state, lent_state)
    lent_stats = lax.ppermute(stats, "y", [(1, 0)])
    prefix_share = sum_parts(grads, SEQ).astype(BF16)
    prefix_grads = to_all(prefix_share, SEQ).reshape(2, npre, HD)
    lent_grad = ()
    for piece in range(PIECES):
        lent_grad = (
            query_grad_piece(True, piece, pos, lent_q, lent_g, lent_stats, mine, other, *lent_grad),
        )
    lent_grad = lax.ppermute(*lent_grad, "y", [(0, 1)])
    own_grad = pkv
    for piece in range(PIECES):
        own_grad = query_grad_piece(False, piece, pos, q, g, stats, mine, other, own_grad)
    query_grad = (own_grad.astype(F32) + lent_grad.astype(F32)).astype(BF16)
    grad_w_out = w_out_grad(hidden, prefix_grads)
    hidden_part = jnp.einsum("cpk,hck->ph", prefix_grads, w_out, preferred_element_type=F32)
    parts = exchange(hidden_part.reshape(heads, share, units), HEAD)
    pre_part, embed_part = embed_rows(parts, factor, w_hidden)
    own_embed = jnp.sum(exchange(embed_part, CYZ).astype(F32), axis=0).astype(BF16)
    near = to_all(own_embed, OWNERS)
    far = shift(near, "c", 1)
    grad_prefix = joined(pos, near, far, heads, npre, emb)
    both = jnp.concatenate([pre_part, shift(pre_part, "w", 1)], 0)
    turns = [shift(both, "x", k) for k in range(1, lax.axis_size("x"))]
    grad_w_hidden, grad_b_hidden = w_hidden_grad(place, prefix_embed, both, *turns)
    return (query_grad, grad_w_out, grad_w_hidden, grad_b_hidden, grad_prefix)


def solution(mesh):
    torus = Mesh(mesh.devices.reshape(2, 8, 2, 4, 2), ("y", "z", "c", "x", "w"))
    placed = (
        P(),
        P(None, SEQ),
        P(SEQ),
        P(SEQ, None, HEAD),
        P(SEQ, HEAD),
        P(SEQ, HEAD),
        P(SEQ, HEAD),
        P(SEQ, HEAD),
    )
    return jax.shard_map(
        on_device,
        mesh=torus,
        in_specs=placed,
        out_specs=(P(SEQ, HEAD), P(SEQ, None, HEAD), P(None, SEQ), P(SEQ), P()),
        check_vma=False,
    )
```

```python
import functools
import math

import jax
import jax.numpy as jnp
from jax import lax
from jax.experimental import pallas as pl
from jax.experimental.pallas import tpu as pltpu
from jax.sharding import Mesh
from jax.sharding import PartitionSpec as P

HD = 128
SCALE = 1.0 / math.sqrt(HD)
C1 = SCALE * math.log2(math.e)
NEG = -1e30
TILE = 256
PIECES = 2
TALL = 8
SEQ = ("y", "z", "c")
YZ = ("y", "z")
CYZ = ("c", "y", "z")
HEAD = ("x", "w")
OWNERS = ("x", "w", "y", "z")
F32 = jnp.float32
BF16 = jnp.bfloat16
SMEM = pl.BlockSpec(memory_space=pltpu.SMEM)
VMEM = pl.BlockSpec(memory_space=pltpu.VMEM)
GRANT = 16 * 2**20


def dot_nt(a, b):
    return lax.dot_general(a, b, (((1,), (1,)), ((), ())), preferred_element_type=F32)


def dot_nn(a, b):
    return lax.dot_general(a, b, (((1,), (0,)), ((), ())), preferred_element_type=F32)


def dot_tn(a, b):
    return lax.dot_general(a, b, (((0,), (0,)), ((), ())), preferred_element_type=F32)


def span(r):
    return slice(r * TILE, (r + 1) * TILE)


def update(state, s, d):
    m, l, t = state
    s = s.reshape(-1, 8, TILE)
    d = d.reshape(-1, 8, TILE)
    new = jnp.maximum(m, jnp.max(s, axis=0))
    fade = jnp.exp2(m - new)
    w = jnp.exp2(s - new[None])
    return (new, l * fade + jnp.sum(w, axis=0), t * fade + jnp.sum(w * d, axis=0))


def pair_of(kv, j):
    k = jnp.concatenate([kv[2 * j, :HD], kv[2 * j + 1, :HD]], 0)
    v = jnp.concatenate([kv[2 * j, HD : 2 * HD], kv[2 * j + 1, HD : 2 * HD]], 0)
    return k, v


def visible(pos, own, j, shape, key_dim):
    key = lax.broadcasted_iota(jnp.int32, shape, key_dim)
    row = lax.broadcasted_iota(jnp.int32, shape, 1 - key_dim) % HD
    if own:
        return key <= (pos[0] - 2 * j) * HD + row
    return key < (pos[0] + pos[1] - 2 * j) * HD


def generate_kernel(place, embed, w_hidden, bias, w_out, keys, values, hidden, factor, payload, tangent):
    tangent[...] = jnp.tanh(dot_nn(embed[...], w_hidden[...]) + bias[...])
    hidden[...] = tangent[...].astype(BF16)
    share = factor.shape[0]
    first = pl.multiple_of((2 * place[0] + place[1]) * share, share)
    own = tangent[pl.ds(first, share), :]
    factor[...] = 1.0 - own * own
    groups = payload.shape[0]
    rows = keys.shape[0]
    npre = hidden.shape[0]
    size = 2 * npre // groups
    for c in range(2):
        part = dot_nn(hidden[...], w_out[:, c, :]).astype(BF16)
        for k in range(groups // 2):
            payload[c * groups // 2 + k, 2 * rows :, :] = part[k * size : (k + 1) * size]
    for k in range(groups):
        payload[k, :rows, :] = keys[...]
        payload[k, rows : 2 * rows, :] = values[...]


def generated(place, embed, w_hidden, bias, w_out, keys, values):
    npre, units = embed.shape[0], w_hidden.shape[1]
    groups = lax.axis_size("z")
    out = (
        jax.ShapeDtypeStruct((npre, units), BF16),
        jax.ShapeDtypeStruct((npre // lax.axis_size(HEAD), units), F32),
        jax.ShapeDtypeStruct((groups, 2 * keys.shape[0] + 2 * npre // groups, HD), BF16),
    )
    values_in = (embed, w_hidden, bias, w_out, keys, values)
    return pl.pallas_call(
        generate_kernel,
        out_shape=out,
        in_specs=[SMEM] + [whole(v) for v in values_in],
        out_specs=tuple(whole(v) for v in out),
        grid=(1,),
        scratch_shapes=[pltpu.VMEM((npre, units), F32)],
        compiler_params=pltpu.CompilerParams(vmem_limit_bytes=GRANT),
        cost_estimate=pl.CostEstimate(flops=2 * 10**8, bytes_accessed=2 * 10**6, transcendentals=10**5),
        name="generate",
    )(place, *(pltpu.with_memory_space_constraint(v, pltpu.HBM) for v in values_in))


def whole(value):
    return pl.BlockSpec(value.shape, lambda *_: (0,) * len(value.shape))


def sweep_step(pos, q, g, sources, j, states, masked=False):
    for own, kv in sources:
        k, v = pair_of(kv, j)
        seen = visible(pos, own, j, (2 * HD, TILE), 0) if masked else None
        new = []
        for r in range(q.shape[0] // TILE):
            s = dot_nt(k, q[span(r), :]) * C1
            if masked:
                s = jnp.where(seen, s, NEG)
            new.append(update(states[r], s, dot_nt(v, g[span(r), :])))
        states = tuple(new)
    return states


def empty_states(tiles):
    zero = jnp.zeros((8, TILE), F32)
    return tuple((jnp.full((8, TILE), NEG, F32), zero, zero) for _ in range(tiles))


def sweep_kernel(pos, q, g, mine, other, out):
    tiles = q.shape[0] // TILE
    step = functools.partial(sweep_step, pos, q, g, ((True, mine), (False, other)))
    half = pos[0] // 2
    states = step(half, lax.fori_loop(0, half, step, empty_states(tiles)), True)
    for r in range(tiles):
        for a in range(3):
            out[a, :, span(r)] = states[r][a]


def merged(m, l, t):
    top = jnp.max(m, axis=0, keepdims=True)
    fade = jnp.exp2(m - top)
    return top, jnp.sum(l * fade, axis=0, keepdims=True), jnp.sum(t * fade, axis=0, keepdims=True)


def lent_sweep_kernel(last, pos, q, g, kv, *refs):
    *begun, out = refs
    tiles = q.shape[0] // TILE
    states = empty_states(tiles)
    if begun:
        states = tuple(tuple(begun[0][a, :, span(r)] for a in range(3)) for r in range(tiles))
    step = functools.partial(sweep_step, pos, q, g, ((True, kv),))
    pairs = jnp.where(pos[2] == 0, kv.shape[0] // 2, 0)
    states = lax.fori_loop(0, pairs, step, states)
    for r in range(tiles):
        if last:
            for a, value in enumerate(merged(*states[r])):
                out[a : a + 1, span(r)] = value
        else:
            for a in range(3):
                out[a, :, span(r)] = states[r][a]


def prefix_kernel(pos, q, g, halves, state, lent, grads, stats, pkv):
    npre = pkv.shape[1]
    pkv[...] = (halves[0].astype(F32) + halves[1].astype(F32)).astype(BF16)
    kg = jnp.zeros((npre, HD), F32)
    vg = jnp.zeros((npre, HD), F32)
    late = pos[2] == 1
    for r in range(q.shape[0] // TILE):
        s = dot_nt(pkv[0], q[span(r), :]) * C1
        d = dot_nt(pkv[1], g[span(r), :])
        near = merged(*update(tuple(state[a, :, span(r)] for a in range(3)), s, d))
        far = tuple(
            jnp.where(late, lent[a : a + 1, span(r)], empty) for a, empty in enumerate((NEG, 0.0, 0.0))
        )
        top = jnp.maximum(near[0], far[0])
        near_fade = jnp.exp2(near[0] - top)
        far_fade = jnp.exp2(far[0] - top)
        total = near[1] * near_fade + far[1] * far_fade
        delta = (near[2] * near_fade + far[2] * far_fade) / total
        log_total = top + jnp.log2(total)
        stats[0:1, span(r)] = log_total
        stats[1:2, span(r)] = delta
        p = jnp.exp2(s - log_total)
        kg = kg + dot_nn((p * (d - delta)).astype(BF16), q[span(r), :])
        vg = vg + dot_nn(p.astype(BF16), g[span(r), :])
    grads[0] = (kg * SCALE).astype(grads.dtype)
    grads[1] = vg.astype(grads.dtype)


def grad_kernel(lent, piece, pos, q, g, stats, mine, other, *refs):
    *extra, out, total, log_total, delta = refs[: len(refs) - 2 * (piece > 0)]
    rows = q.shape[0]
    pairs = mine.shape[0] // 2 // PIECES
    first = piece * pairs

    def part(k, v, seen=None):
        for r in range(rows // TILE):
            s = dot_nt(q[span(r), :], k) * C1
            if seen is not None:
                s = jnp.where(seen, s, NEG)
            d = dot_nt(g[span(r), :], v)
            pieces = []
            for b in range(k.shape[0] // HD):
                lanes = slice(b * HD, (b + 1) * HD)
                p = jnp.exp2(s[:, lanes] - log_total[span(r), :])
                pieces.append((p * (d[:, lanes] - delta[span(r), :])).astype(BF16))
            total[span(r), :] += dot_nn(jnp.concatenate(pieces, 1), k)

    def step(i, masked=False):
        for own, kv in ((True, mine), (False, other)):
            k, v = pair_of(kv, first + i)
            seen = visible(pos, own, first + i, (TILE, 2 * HD), 1) if masked else None
            part(k, v, seen)

    def spread():
        columns = stats[...].T
        log_total[...] = jnp.broadcast_to(columns[:, 0:1], (rows, HD))
        delta[...] = jnp.broadcast_to(columns[:, 1:2], (rows, HD))

    if piece > 0:
        held, sem = refs[-2:]
        copy = pltpu.make_async_copy(extra[0], held, sem)
        copy.start()
    total[...] = jnp.zeros((rows, HD), F32)
    if lent:

        @pl.when(pos[2] == 0)
        def _():
            spread()
            lax.fori_loop(0, pairs, lambda i, _: step(i), None)

    else:
        spread()
        if piece == 0:
            part(extra[0][0], extra[0][1])
        half = pos[0] // 2
        lax.fori_loop(0, jnp.clip(half - first, 0, pairs), lambda i, _: step(i), None)

        @pl.when((half >= first) & (half < first + pairs))
        def _():
            step(half - first, True)

    if piece > 0:
        copy.wait()
    for h in range(rows // HD):
        at = slice(h * HD, (h + 1) * HD)
        result = total[at, :] * SCALE
        if piece > 0:
            result = result + held[:, at].astype(F32)
        out[:, at] = result.astype(out.dtype)


def call(kernel, out_shape, flops, *values, far=(), scratch=()):
    spaces = [pltpu.SMEM if v.dtype == jnp.int32 else pltpu.VMEM for v in values]
    spaces += [pltpu.HBM for _ in far]
    held = [
        v if space == pltpu.SMEM else pltpu.with_memory_space_constraint(v, space)
        for v, space in zip((*values, *far), spaces)
    ]
    return pl.pallas_call(
        kernel,
        out_shape=out_shape,
        in_specs=[pl.BlockSpec(memory_space=space) for space in spaces],
        out_specs=jax.tree.map(lambda _: VMEM, out_shape),
        scratch_shapes=list(scratch),
        compiler_params=pltpu.CompilerParams(vmem_limit_bytes=GRANT),
        cost_estimate=pl.CostEstimate(flops=flops, bytes_accessed=10**6, transcendentals=10**6),
    )(*held)


def sweep(pos, q, g, mine, other):
    return call(sweep_kernel, jax.ShapeDtypeStruct((3, 8, q.shape[0]), F32), 10**9, pos, q, g, mine, other)


def lent_sweep(pos, q, g, kv, *begun):
    last = bool(begun)
    out = jax.ShapeDtypeStruct((3, q.shape[0]) if last else (3, 8, q.shape[0]), F32)
    kernel = functools.partial(lent_sweep_kernel, last)
    return call(kernel, out, 5 * 10**8, pos, q, g, kv, *begun)


def prefix_part(pos, q, g, halves, state, lent):
    pair = jax.ShapeDtypeStruct(halves.shape[1:], BF16)
    out = (pair, jax.ShapeDtypeStruct((2, q.shape[0]), F32), pair)
    return call(prefix_kernel, out, 3 * 10**8, pos, q, g, halves, state, lent)


def query_grad_piece(lent, piece, pos, q, g, stats, mine, other, *extra):
    out = jax.ShapeDtypeStruct(q.shape[::-1], BF16)
    scratch = [pltpu.VMEM(q.shape, F32)] * 3
    far = ()
    if piece > 0:
        far, extra = extra, ()
        scratch += [pltpu.VMEM(q.shape[::-1], BF16), pltpu.SemaphoreType.DMA]
    kernel = functools.partial(grad_kernel, lent, piece)
    return call(kernel, out, 10**9, pos, q, g, stats, mine, other, *extra, far=far, scratch=scratch)


def embed_kernel(parts, factor, w_hidden, pre, embed):
    pre[...] = (jnp.sum(parts[...], axis=0) * factor[...]).astype(BF16)
    rows = dot_nt(pre[...], w_hidden[...])
    tall = embed.shape[1]
    wide = rows.shape[1] // HD
    for t in range(embed.shape[0]):
        down, right = t // wide * tall, t % wide * HD
        embed[t] = rows[down : down + tall, right : right + HD].astype(BF16)


def embed_rows(parts, factor, w_hidden):
    share = factor.shape[0]
    out = (
        jax.ShapeDtypeStruct(factor.shape, BF16),
        jax.ShapeDtypeStruct((share * w_hidden.shape[0] // HD // TALL, TALL, HD), BF16),
    )
    return call(embed_kernel, out, 2 * 10**7, parts, factor, w_hidden)


def joined_kernel(heads, pos, near, far, out):
    wide = out.shape[1] // HD
    per_head = near.shape[0] // heads
    first = pos[1] == 0
    for t in range(near.shape[0]):
        pair = (near[t].astype(F32), far[t].astype(F32))
        for side in range(2):
            tile = t // per_head * 2 * per_head + side * per_head + t % per_head
            down, right = tile // wide * TALL, tile % wide * HD
            value = jnp.where(first, pair[side], pair[1 - side])
            out[down : down + TALL, right : right + HD] = value


def joined(pos, near, far, heads, npre, emb):
    out = jax.ShapeDtypeStruct((npre, emb), F32)
    return call(functools.partial(joined_kernel, heads), out, 10**6, pos, near, far)


def w_hidden_kernel(place, embed, *refs):
    *parts, grad_w, grad_b, pre = refs
    lines = len(parts)
    share = parts[0].shape[0] // 2
    for k, part in enumerate(parts):
        line = (place[0] + lines - k) % lines
        for side in range(2):
            source = 2 * line + (place[1] + side) % 2
            pre[pl.ds(pl.multiple_of(source * share, share), share), :] = part[side * share : (side + 1) * share]
    grad_w[...] = dot_tn(embed[...], pre[...])
    grad_b[...] = jnp.sum(pre[...].astype(F32), axis=0)


def w_hidden_grad(place, embed, *parts):
    npre, emb = embed.shape
    units = parts[0].shape[1]
    out = (jax.ShapeDtypeStruct((emb, units), F32), jax.ShapeDtypeStruct((units,), F32))
    scratch = [pltpu.VMEM((npre, units), BF16)]
    return call(w_hidden_kernel, out, 2 * 10**8, place, embed, *parts, scratch=scratch)


def w_out_kernel(hidden, grads, out):
    for c in range(grads.shape[0]):
        out[:, c, :] = dot_tn(hidden[...], grads[c])


def w_out_grad(hidden, grads):
    out = jax.ShapeDtypeStruct((hidden.shape[1], grads.shape[0], HD), F32)
    return call(w_out_kernel, out, 10**8, hidden, grads)


def exchange(value, axes):
    return lax.all_to_all(value, axes, 0, 0, tiled=True)


def to_all(value, axes):
    return exchange(jnp.broadcast_to(value, (lax.axis_size(axes), *value.shape)), axes)


def sum_parts(value, axes, dtype=BF16):
    parts = exchange(value.reshape(lax.axis_size(axes), -1, HD).astype(dtype), axes)
    return jnp.sum(parts.astype(F32), axis=0)


def shift(value, axis, steps):
    count = lax.axis_size(axis)
    return lax.ppermute(value, axis, [(i, (i + steps) % count) for i in range(count)])


def by_head(rows):
    return rows.reshape(rows.shape[0], -1, HD).transpose(1, 0, 2).reshape(-1, HD)


def on_device(prefix_embed, w_hidden, b_hidden, w_out, queries, keys, values, out_grad):
    npre, emb = prefix_embed.shape
    units = w_hidden.shape[1]
    core = lax.axis_index("c")
    late = lax.axis_index("y")
    heads = lax.axis_size(HEAD)
    share = npre // heads
    place = jnp.stack([lax.axis_index("x"), lax.axis_index("w")]).astype(jnp.int32)
    pos = jnp.stack([lax.axis_index("z"), core, late]).astype(jnp.int32)

    hidden, factor, payload = generated(
        place, prefix_embed, w_hidden, b_hidden.reshape(1, units), w_out, keys, values
    )
    kv_rows = 2 * keys.shape[0]
    mine = exchange(payload, "z")
    q = by_head(queries)
    g = by_head(out_grad)
    lent_q = lax.ppermute(queries, "y", [(1, 0)])
    lent_g = lax.ppermute(out_grad, "y", [(1, 0)])
    lent_q = by_head(lent_q)
    lent_g = by_head(lent_g)
    other = shift(mine, "c", 1)
    lent_state = lent_sweep(pos, lent_q, lent_g, mine)
    sides = [jnp.sum(v[:, kv_rows:].astype(F32), axis=0) for v in (mine, other)]
    own = (sides[0] + sides[1]).astype(BF16)
    halves = to_all(own, YZ).reshape(lax.axis_size("y"), 2, npre, HD)
    lent_state = lent_sweep(pos, lent_q, lent_g, other, lent_state)
    lent_state = lax.ppermute(lent_state, "y", [(0, 1)])
    state = sweep(pos, q, g, mine, other)
    grads, stats, pkv = prefix_part(pos, q, g, halves, state, lent_state)
    lent_stats = lax.ppermute(stats, "y", [(1, 0)])
    prefix_share = sum_parts(grads, SEQ).astype(BF16)
    prefix_grads = to_all(prefix_share, SEQ).reshape(2, npre, HD)
    lent_grad = ()
    for piece in range(PIECES):
        lent_grad = (
            query_grad_piece(True, piece, pos, lent_q, lent_g, lent_stats, mine, other, *lent_grad),
        )
    lent_grad = lax.ppermute(*lent_grad, "y", [(0, 1)])
    own_grad = pkv
    for piece in range(PIECES):
        own_grad = query_grad_piece(False, piece, pos, q, g, stats, mine, other, own_grad)
    query_grad = (own_grad.astype(F32) + lent_grad.astype(F32)).astype(BF16)
    grad_w_out = w_out_grad(hidden, prefix_grads)
    hidden_part = jnp.einsum("cpk,hck->ph", prefix_grads, w_out, preferred_element_type=F32)
    parts = exchange(hidden_part.reshape(heads, share, units), HEAD)
    pre_part, embed_part = embed_rows(parts, factor, w_hidden)
    own_embed = jnp.sum(exchange(embed_part, CYZ).astype(F32), axis=0).astype(BF16)
    near = to_all(own_embed, OWNERS)
    far = shift(near, "c", 1)
    grad_prefix = joined(pos, near, far, heads, npre, emb)
    both = jnp.concatenate([pre_part, shift(pre_part, "w", 1)], 0)
    turns = [shift(both, "x", k) for k in range(1, lax.axis_size("x"))]
    grad_w_hidden, grad_b_hidden = w_hidden_grad(place, prefix_embed, both, *turns)
    return (query_grad, grad_w_out, grad_w_hidden, grad_b_hidden, grad_prefix)


def solution(mesh):
    torus = Mesh(mesh.devices.reshape(2, 8, 2, 4, 2), ("y", "z", "c", "x", "w"))
    placed = (
        P(),
        P(None, SEQ),
        P(SEQ),
        P(SEQ, None, HEAD),
        P(SEQ, HEAD),
        P(SEQ, HEAD),
        P(SEQ, HEAD),
        P(SEQ, HEAD),
    )
    return jax.shard_map(
        on_device,
        mesh=torus,
        in_specs=placed,
        out_specs=(P(SEQ, HEAD), P(SEQ, None, HEAD), P(None, SEQ), P(SEQ), P()),
        check_vma=False,
    )
```

```python
import functools
import math

import jax
import jax.numpy as jnp
from jax import lax
from jax.experimental import pallas as pl
from jax.experimental.pallas import tpu as pltpu
from jax.sharding import Mesh
from jax.sharding import PartitionSpec as P

HD = 128
SCALE = 1.0 / math.sqrt(HD)
C1 = SCALE * math.log2(math.e)
NEG = -1e30
TILE = 256
PIECES = 2
TALL = 8
SEQ = ("y", "z", "c")
YZ = ("y", "z")
CYZ = ("c", "y", "z")
HEAD = ("x", "w")
OWNERS = ("x", "w", "y", "z")
F32 = jnp.float32
BF16 = jnp.bfloat16
SMEM = pl.BlockSpec(memory_space=pltpu.SMEM)
VMEM = pl.BlockSpec(memory_space=pltpu.VMEM)
GRANT = 16 * 2**20


def dot_nt(a, b):
    return lax.dot_general(a, b, (((1,), (1,)), ((), ())), preferred_element_type=F32)


def dot_nn(a, b):
    return lax.dot_general(a, b, (((1,), (0,)), ((), ())), preferred_element_type=F32)


def dot_tn(a, b):
    return lax.dot_general(a, b, (((0,), (0,)), ((), ())), preferred_element_type=F32)


def span(r):
    return slice(r * TILE, (r + 1) * TILE)


def update(state, s, d):
    m, l, t = state
    s = s.reshape(-1, 8, TILE)
    d = d.reshape(-1, 8, TILE)
    new = jnp.maximum(m, jnp.max(s, axis=0))
    fade = jnp.exp2(m - new)
    w = jnp.exp2(s - new[None])
    return (new, l * fade + jnp.sum(w, axis=0), t * fade + jnp.sum(w * d, axis=0))


def pair_of(kv, j):
    k = jnp.concatenate([kv[2 * j, :HD], kv[2 * j + 1, :HD]], 0)
    v = jnp.concatenate([kv[2 * j, HD : 2 * HD], kv[2 * j + 1, HD : 2 * HD]], 0)
    return k, v


def visible(pos, own, j, shape, key_dim):
    key = lax.broadcasted_iota(jnp.int32, shape, key_dim)
    row = lax.broadcasted_iota(jnp.int32, shape, 1 - key_dim) % HD
    if own:
        return key <= (pos[0] - 2 * j) * HD + row
    return key < (pos[0] + pos[1] - 2 * j) * HD


def generate_kernel(place, embed, w_hidden, bias, w_out, keys, values, hidden, factor, payload, tangent):
    tangent[...] = jnp.tanh(dot_nn(embed[...], w_hidden[...]) + bias[...])
    hidden[...] = tangent[...].astype(BF16)
    share = factor.shape[0]
    first = pl.multiple_of((2 * place[0] + place[1]) * share, share)
    own = tangent[pl.ds(first, share), :]
    factor[...] = 1.0 - own * own
    groups = payload.shape[0]
    rows = keys.shape[0]
    npre = hidden.shape[0]
    size = 2 * npre // groups
    for c in range(2):
        part = dot_nn(hidden[...], w_out[:, c, :]).astype(BF16)
        for k in range(groups // 2):
            payload[c * groups // 2 + k, 2 * rows :, :] = part[k * size : (k + 1) * size]
    for k in range(groups):
        payload[k, :rows, :] = keys[...]
        payload[k, rows : 2 * rows, :] = values[...]


def generated(place, embed, w_hidden, bias, w_out, keys, values):
    npre, units = embed.shape[0], w_hidden.shape[1]
    groups = lax.axis_size("z")
    out = (
        jax.ShapeDtypeStruct((npre, units), BF16),
        jax.ShapeDtypeStruct((npre // lax.axis_size(HEAD), units), F32),
        jax.ShapeDtypeStruct((groups, 2 * keys.shape[0] + 2 * npre // groups, HD), BF16),
    )
    values_in = (embed, w_hidden, bias, w_out, keys, values)
    return pl.pallas_call(
        generate_kernel,
        out_shape=out,
        in_specs=[SMEM] + [whole(v) for v in values_in],
        out_specs=tuple(whole(v) for v in out),
        grid=(1,),
        scratch_shapes=[pltpu.VMEM((npre, units), F32)],
        compiler_params=pltpu.CompilerParams(vmem_limit_bytes=GRANT),
        cost_estimate=pl.CostEstimate(flops=2 * 10**8, bytes_accessed=2 * 10**6, transcendentals=10**5),
        name="generate",
    )(place, *(pltpu.with_memory_space_constraint(v, pltpu.HBM) for v in values_in))


def whole(value):
    return pl.BlockSpec(value.shape, lambda *_: (0,) * len(value.shape))


def sweep_step(pos, q, g, sources, j, states, masked=False):
    for own, kv in sources:
        k, v = pair_of(kv, j)
        seen = visible(pos, own, j, (2 * HD, TILE), 0) if masked else None
        new = []
        for r in range(q.shape[0] // TILE):
            s = dot_nt(k, q[span(r), :]) * C1
            if masked:
                s = jnp.where(seen, s, NEG)
            new.append(update(states[r], s, dot_nt(v, g[span(r), :])))
        states = tuple(new)
    return states


def empty_states(tiles):
    zero = jnp.zeros((8, TILE), F32)
    return tuple((jnp.full((8, TILE), NEG, F32), zero, zero) for _ in range(tiles))


def sweep_kernel(pos, q, g, mine, other, out):
    tiles = q.shape[0] // TILE
    step = functools.partial(sweep_step, pos, q, g, ((True, mine), (False, other)))
    half = pos[0] // 2
    states = step(half, lax.fori_loop(0, half, step, empty_states(tiles)), True)
    for r in range(tiles):
        for a in range(3):
            out[a, :, span(r)] = states[r][a]


def merged(m, l, t):
    top = jnp.max(m, axis=0, keepdims=True)
    fade = jnp.exp2(m - top)
    return top, jnp.sum(l * fade, axis=0, keepdims=True), jnp.sum(t * fade, axis=0, keepdims=True)


def lent_sweep_kernel(last, pos, q, g, kv, *refs):
    *begun, out = refs
    tiles = q.shape[0] // TILE
    states = empty_states(tiles)
    if begun:
        states = tuple(tuple(begun[0][a, :, span(r)] for a in range(3)) for r in range(tiles))
    step = functools.partial(sweep_step, pos, q, g, ((True, kv),))
    pairs = jnp.where(pos[2] == 0, kv.shape[0] // 2, 0)
    states = lax.fori_loop(0, pairs, step, states)
    for r in range(tiles):
        if last:
            for a, value in enumerate(merged(*states[r])):
                out[a : a + 1, span(r)] = value
        else:
            for a in range(3):
                out[a, :, span(r)] = states[r][a]


def prefix_kernel(pos, q, g, halves, state, lent, grads, stats, pkv):
    npre = pkv.shape[1]
    pkv[...] = (halves[0].astype(F32) + halves[1].astype(F32)).astype(BF16)
    kg = jnp.zeros((npre, HD), F32)
    vg = jnp.zeros((npre, HD), F32)
    late = pos[2] == 1
    for r in range(q.shape[0] // TILE):
        s = dot_nt(pkv[0], q[span(r), :]) * C1
        d = dot_nt(pkv[1], g[span(r), :])
        near = merged(*update(tuple(state[a, :, span(r)] for a in range(3)), s, d))
        far = tuple(
            jnp.where(late, lent[a : a + 1, span(r)], empty) for a, empty in enumerate((NEG, 0.0, 0.0))
        )
        top = jnp.maximum(near[0], far[0])
        near_fade = jnp.exp2(near[0] - top)
        far_fade = jnp.exp2(far[0] - top)
        total = near[1] * near_fade + far[1] * far_fade
        delta = (near[2] * near_fade + far[2] * far_fade) / total
        log_total = top + jnp.log2(total)
        stats[0:1, span(r)] = log_total
        stats[1:2, span(r)] = delta
        p = jnp.exp2(s - log_total)
        kg = kg + dot_nn((p * (d - delta)).astype(BF16), q[span(r), :])
        vg = vg + dot_nn(p.astype(BF16), g[span(r), :])
    grads[0] = (kg * SCALE).astype(grads.dtype)
    grads[1] = vg.astype(grads.dtype)


def grad_kernel(lent, piece, pos, q, g, stats, mine, other, *refs):
    *extra, out, total, log_total, delta = refs[: len(refs) - 2 * (piece > 0)]
    rows = q.shape[0]
    pairs = mine.shape[0] // 2 // PIECES
    first = piece * pairs

    def part(k, v, seen=None):
        for r in range(rows // TILE):
            s = dot_nt(q[span(r), :], k) * C1
            if seen is not None:
                s = jnp.where(seen, s, NEG)
            d = dot_nt(g[span(r), :], v)
            pieces = []
            for b in range(k.shape[0] // HD):
                lanes = slice(b * HD, (b + 1) * HD)
                p = jnp.exp2(s[:, lanes] - log_total[span(r), :])
                pieces.append((p * (d[:, lanes] - delta[span(r), :])).astype(BF16))
            total[span(r), :] += dot_nn(jnp.concatenate(pieces, 1), k)

    def step(i, masked=False):
        for own, kv in ((True, mine), (False, other)):
            k, v = pair_of(kv, first + i)
            seen = visible(pos, own, first + i, (TILE, 2 * HD), 1) if masked else None
            part(k, v, seen)

    def spread():
        columns = stats[...].T
        log_total[...] = jnp.broadcast_to(columns[:, 0:1], (rows, HD))
        delta[...] = jnp.broadcast_to(columns[:, 1:2], (rows, HD))

    if piece > 0:
        held, sem = refs[-2:]
        copy = pltpu.make_async_copy(extra[0], held, sem)
        copy.start()
    total[...] = jnp.zeros((rows, HD), F32)
    if lent:

        @pl.when(pos[2] == 0)
        def _():
            spread()
            lax.fori_loop(0, pairs, lambda i, _: step(i), None)

    else:
        spread()
        if piece == 0:
            part(extra[0][0], extra[0][1])
        half = pos[0] // 2
        lax.fori_loop(0, jnp.clip(half - first, 0, pairs), lambda i, _: step(i), None)

        @pl.when((half >= first) & (half < first + pairs))
        def _():
            step(half - first, True)

    if piece > 0:
        copy.wait()
    for h in range(rows // HD):
        at = slice(h * HD, (h + 1) * HD)
        result = total[at, :] * SCALE
        if piece > 0:
            result = result + held[:, at].astype(F32)
        out[:, at] = result.astype(out.dtype)


def call(kernel, out_shape, flops, *values, far=(), scratch=()):
    spaces = [pltpu.SMEM if v.dtype == jnp.int32 else pltpu.VMEM for v in values]
    spaces += [pltpu.HBM for _ in far]
    held = [
        v if space == pltpu.SMEM else pltpu.with_memory_space_constraint(v, space)
        for v, space in zip((*values, *far), spaces)
    ]
    return pl.pallas_call(
        kernel,
        out_shape=out_shape,
        in_specs=[pl.BlockSpec(memory_space=space) for space in spaces],
        out_specs=jax.tree.map(lambda _: VMEM, out_shape),
        scratch_shapes=list(scratch),
        compiler_params=pltpu.CompilerParams(vmem_limit_bytes=GRANT),
        cost_estimate=pl.CostEstimate(flops=flops, bytes_accessed=10**6, transcendentals=10**6),
    )(*held)


def sweep(pos, q, g, mine, other):
    return call(sweep_kernel, jax.ShapeDtypeStruct((3, 8, q.shape[0]), F32), 10**9, pos, q, g, mine, other)


def lent_sweep(pos, q, g, kv, *begun):
    last = bool(begun)
    out = jax.ShapeDtypeStruct((3, q.shape[0]) if last else (3, 8, q.shape[0]), F32)
    kernel = functools.partial(lent_sweep_kernel, last)
    return call(kernel, out, 5 * 10**8, pos, q, g, kv, *begun)


def prefix_part(pos, q, g, halves, state, lent):
    pair = jax.ShapeDtypeStruct(halves.shape[1:], BF16)
    out = (pair, jax.ShapeDtypeStruct((2, q.shape[0]), F32), pair)
    return call(prefix_kernel, out, 3 * 10**8, pos, q, g, halves, state, lent)


def query_grad_piece(lent, piece, pos, q, g, stats, mine, other, *extra):
    out = jax.ShapeDtypeStruct(q.shape[::-1], BF16)
    scratch = [pltpu.VMEM(q.shape, F32)] * 3
    far = ()
    if piece > 0:
        far, extra = extra, ()
        scratch += [pltpu.VMEM(q.shape[::-1], BF16), pltpu.SemaphoreType.DMA]
    kernel = functools.partial(grad_kernel, lent, piece)
    return call(kernel, out, 10**9, pos, q, g, stats, mine, other, *extra, far=far, scratch=scratch)


def embed_kernel(parts, factor, w_hidden, pre, embed):
    pre[...] = (jnp.sum(parts[...], axis=0) * factor[...]).astype(BF16)
    rows = dot_nt(pre[...], w_hidden[...])
    tall = embed.shape[1]
    wide = rows.shape[1] // HD
    for t in range(embed.shape[0]):
        down, right = t // wide * tall, t % wide * HD
        embed[t] = rows[down : down + tall, right : right + HD].astype(BF16)


def embed_rows(parts, factor, w_hidden):
    share = factor.shape[0]
    out = (
        jax.ShapeDtypeStruct(factor.shape, BF16),
        jax.ShapeDtypeStruct((share * w_hidden.shape[0] // HD // TALL, TALL, HD), BF16),
    )
    return call(embed_kernel, out, 2 * 10**7, parts, factor, w_hidden)


def joined_kernel(heads, pos, near, far, out):
    wide = out.shape[1] // HD
    per_head = near.shape[0] // heads
    deep = per_head // wide * TALL
    for side, source in ((pos[1], near), (1 - pos[1], far)):
        for t in range(near.shape[0]):
            down = t // per_head * 2 * deep + t % per_head // wide * TALL
            at = pl.multiple_of(down + side * deep, TALL)
            right = t % wide * HD
            out[pl.ds(at, TALL), right : right + HD] = source[t].astype(F32)


def joined(pos, near, far, heads, npre, emb):
    out = jax.ShapeDtypeStruct((npre, emb), F32)
    return call(functools.partial(joined_kernel, heads), out, 10**6, pos, near, far)


def w_hidden_kernel(place, embed, *refs):
    *parts, grad_w, grad_b, pre = refs
    lines = len(parts)
    share = parts[0].shape[0] // 2
    for k, part in enumerate(parts):
        line = (place[0] + lines - k) % lines
        for side in range(2):
            source = 2 * line + (place[1] + side) % 2
            pre[pl.ds(pl.multiple_of(source * share, share), share), :] = part[side * share : (side + 1) * share]
    grad_w[...] = dot_tn(embed[...], pre[...])
    grad_b[...] = jnp.sum(pre[...].astype(F32), axis=0)


def w_hidden_grad(place, embed, *parts):
    npre, emb = embed.shape
    units = parts[0].shape[1]
    out = (jax.ShapeDtypeStruct((emb, units), F32), jax.ShapeDtypeStruct((units,), F32))
    scratch = [pltpu.VMEM((npre, units), BF16)]
    return call(w_hidden_kernel, out, 2 * 10**8, place, embed, *parts, scratch=scratch)


def w_out_kernel(hidden, grads, out):
    for c in range(grads.shape[0]):
        out[:, c, :] = dot_tn(hidden[...], grads[c])


def w_out_grad(hidden, grads):
    out = jax.ShapeDtypeStruct((hidden.shape[1], grads.shape[0], HD), F32)
    return call(w_out_kernel, out, 10**8, hidden, grads)


def exchange(value, axes):
    return lax.all_to_all(value, axes, 0, 0, tiled=True)


def to_all(value, axes):
    return exchange(jnp.broadcast_to(value, (lax.axis_size(axes), *value.shape)), axes)


def sum_parts(value, axes, dtype=BF16):
    parts = exchange(value.reshape(lax.axis_size(axes), -1, HD).astype(dtype), axes)
    return jnp.sum(parts.astype(F32), axis=0)


def shift(value, axis, steps):
    count = lax.axis_size(axis)
    return lax.ppermute(value, axis, [(i, (i + steps) % count) for i in range(count)])


def by_head(rows):
    return rows.reshape(rows.shape[0], -1, HD).transpose(1, 0, 2).reshape(-1, HD)


def on_device(prefix_embed, w_hidden, b_hidden, w_out, queries, keys, values, out_grad):
    npre, emb = prefix_embed.shape
    units = w_hidden.shape[1]
    core = lax.axis_index("c")
    late = lax.axis_index("y")
    heads = lax.axis_size(HEAD)
    share = npre // heads
    place = jnp.stack([lax.axis_index("x"), lax.axis_index("w")]).astype(jnp.int32)
    pos = jnp.stack([lax.axis_index("z"), core, late]).astype(jnp.int32)

    hidden, factor, payload = generated(
        place, prefix_embed, w_hidden, b_hidden.reshape(1, units), w_out, keys, values
    )
    kv_rows = 2 * keys.shape[0]
    mine = exchange(payload, "z")
    q = by_head(queries)
    g = by_head(out_grad)
    lent_q = lax.ppermute(queries, "y", [(1, 0)])
    lent_g = lax.ppermute(out_grad, "y", [(1, 0)])
    lent_q = by_head(lent_q)
    lent_g = by_head(lent_g)
    other = shift(mine, "c", 1)
    lent_state = lent_sweep(pos, lent_q, lent_g, mine)
    sides = [jnp.sum(v[:, kv_rows:].astype(F32), axis=0) for v in (mine, other)]
    own = (sides[0] + sides[1]).astype(BF16)
    halves = to_all(own, YZ).reshape(lax.axis_size("y"), 2, npre, HD)
    lent_state = lent_sweep(pos, lent_q, lent_g, other, lent_state)
    lent_state = lax.ppermute(lent_state, "y", [(0, 1)])
    state = sweep(pos, q, g, mine, other)
    grads, stats, pkv = prefix_part(pos, q, g, halves, state, lent_state)
    lent_stats = lax.ppermute(stats, "y", [(1, 0)])
    prefix_share = sum_parts(grads, SEQ).astype(BF16)
    prefix_grads = to_all(prefix_share, SEQ).reshape(2, npre, HD)
    lent_grad = ()
    for piece in range(PIECES):
        lent_grad = (
            query_grad_piece(True, piece, pos, lent_q, lent_g, lent_stats, mine, other, *lent_grad),
        )
    lent_grad = lax.ppermute(*lent_grad, "y", [(0, 1)])
    own_grad = pkv
    for piece in range(PIECES):
        own_grad = query_grad_piece(False, piece, pos, q, g, stats, mine, other, own_grad)
    query_grad = (own_grad.astype(F32) + lent_grad.astype(F32)).astype(BF16)
    grad_w_out = w_out_grad(hidden, prefix_grads)
    hidden_part = jnp.einsum("cpk,hck->ph", prefix_grads, w_out, preferred_element_type=F32)
    parts = exchange(hidden_part.reshape(heads, share, units), HEAD)
    pre_part, embed_part = embed_rows(parts, factor, w_hidden)
    own_embed = jnp.sum(exchange(embed_part, CYZ).astype(F32), axis=0).astype(BF16)
    near = to_all(own_embed, OWNERS)
    far = shift(near, "c", 1)
    grad_prefix = joined(pos, near, far, heads, npre, emb)
    both = jnp.concatenate([pre_part, shift(pre_part, "w", 1)], 0)
    turns = [shift(both, "x", k) for k in range(1, lax.axis_size("x"))]
    grad_w_hidden, grad_b_hidden = w_hidden_grad(place, prefix_embed, both, *turns)
    return (query_grad, grad_w_out, grad_w_hidden, grad_b_hidden, grad_prefix)


def solution(mesh):
    torus = Mesh(mesh.devices.reshape(2, 8, 2, 4, 2), ("y", "z", "c", "x", "w"))
    placed = (
        P(),
        P(None, SEQ),
        P(SEQ),
        P(SEQ, None, HEAD),
        P(SEQ, HEAD),
        P(SEQ, HEAD),
        P(SEQ, HEAD),
        P(SEQ, HEAD),
    )
    return jax.shard_map(
        on_device,
        mesh=torus,
        in_specs=placed,
        out_specs=(P(SEQ, HEAD), P(SEQ, None, HEAD), P(None, SEQ), P(SEQ), P()),
        check_vma=False,
    )
```
